32 devices in a mesh: dp: 1 (over z), cp: 32 (over y, x, core).
Axes of the slice: x: 4, y: 4, z: 1, core: 2. Of those that a mesh axis runs over, the one named last changes fastest.
The devices are a block of a 4x4x8 slice.
Arguments:
- x_in: bfloat16 [16384, 3584], P(('dp', 'cp'))
- dy_in: bfloat16 [16384, 3584], P(('dp', 'cp'))
- doc_id: int32 [16384], P(('dp', 'cp'))
- w_q: bfloat16 [3584, 2, 256], replicated
- w_k: bfloat16 [3584, 1, 256], replicated
- w_v: bfloat16 [3584, 1, 256], replicated
- w_o: bfloat16 [2, 256, 3584], replicated
Outputs:
- output 1: bfloat16 [16384, 3584], P(('dp', 'cp'))
- output 2: bfloat16 [16384, 3584], P(('dp', 'cp'))
All inputs are finite; a program needn't handle non-finite values.
Results may differ from the reference program's by a relative error of at most 0.0092049.
Values are sent between devices in bfloat16 or wider.
A program may use at most 768 MiB of HBM per device.

```python
import jax
import jax.numpy as jnp
from jax import lax

D_MODEL = 3584
Q_HEADS = 2
KV_HEADS = 1
HEAD_DIM = 256
TOK_DEV = 512
GROUP_DEVS = 32
SEQ_LEN = GROUP_DEVS * TOK_DEV
PIECE_LEN = TOK_DEV // 2
QUERY_GROUP = Q_HEADS // KV_HEADS
DOC_CUTS = max(1, GROUP_DEVS // 2)
NEG_BIG = -1.0e30


def stored_positions():
    row_idx = jnp.arange(SEQ_LEN, dtype=jnp.int32)
    owner_dev = row_idx // TOK_DEV
    offset = row_idx % TOK_DEV
    piece_idx = jnp.where(offset < PIECE_LEN, owner_dev, 2 * GROUP_DEVS - 1 - owner_dev)
    return piece_idx * PIECE_LEN + offset % PIECE_LEN


def setup_inputs(seed: int = 0, part: int = 0) -> dict:
    part_key = jax.random.fold_in(jax.random.key(seed), part)
    key_x, key_dy, key_doc = jax.random.split(part_key, 3)
    key_q, key_k, key_v, key_o = jax.random.split(jax.random.key(seed + 1), 4)
    in_scale = D_MODEL ** -0.5
    out_scale = (Q_HEADS * HEAD_DIM) ** -0.5
    x_in = jax.random.normal(key_x, (SEQ_LEN, D_MODEL), jnp.float32).astype(jnp.bfloat16)
    dy_in = jax.random.normal(key_dy, (SEQ_LEN, D_MODEL), jnp.float32).astype(jnp.bfloat16)
    cut_pos = jax.random.randint(key_doc, (DOC_CUTS,), 1, SEQ_LEN, dtype=jnp.int32)
    doc_id = jnp.sum((stored_positions()[:, None] >= cut_pos[None, :]).astype(jnp.int32), axis=1)
    w_q = (jax.random.normal(key_q, (D_MODEL, Q_HEADS, HEAD_DIM), jnp.float32) * in_scale).astype(jnp.bfloat16)
    w_k = (jax.random.normal(key_k, (D_MODEL, KV_HEADS, HEAD_DIM), jnp.float32) * in_scale).astype(jnp.bfloat16)
    w_v = (jax.random.normal(key_v, (D_MODEL, KV_HEADS, HEAD_DIM), jnp.float32) * in_scale).astype(jnp.bfloat16)
    w_o = (jax.random.normal(key_o, (Q_HEADS, HEAD_DIM, D_MODEL), jnp.float32) * out_scale).astype(jnp.bfloat16)
    return {'x_in': x_in, 'dy_in': dy_in, 'doc_id': doc_id, 'w_q': w_q, 'w_k': w_k, 'w_v': w_v, 'w_o': w_o}


def reference(x_in, dy_in, doc_id, w_q, w_k, w_v, w_o):
    score_scale = HEAD_DIM ** -0.5
    all_pos = stored_positions()
    wq_flat = w_q.reshape(D_MODEL, Q_HEADS * HEAD_DIM)
    wk_flat = w_k.reshape(D_MODEL, KV_HEADS * HEAD_DIM)
    wv_flat = w_v.reshape(D_MODEL, KV_HEADS * HEAD_DIM)
    wo_flat = w_o.reshape(Q_HEADS * HEAD_DIM, D_MODEL)
    q_all = jnp.dot(x_in, wq_flat, preferred_element_type=jnp.float32).astype(jnp.bfloat16)
    q_all = q_all.reshape(SEQ_LEN, KV_HEADS, QUERY_GROUP, HEAD_DIM)
    k_all = jnp.dot(x_in, wk_flat, preferred_element_type=jnp.float32).astype(jnp.bfloat16)
    v_all = jnp.dot(x_in, wv_flat, preferred_element_type=jnp.float32).astype(jnp.bfloat16)
    k_wide = k_all.reshape(SEQ_LEN, KV_HEADS, HEAD_DIM).astype(jnp.float32)
    v_wide = v_all.reshape(SEQ_LEN, KV_HEADS, HEAD_DIM).astype(jnp.float32)
    do_all = jnp.dot(dy_in, wo_flat.T, preferred_element_type=jnp.float32).astype(jnp.bfloat16)
    do_all = do_all.reshape(SEQ_LEN, KV_HEADS, QUERY_GROUP, HEAD_DIM)

    def block_step(grad_acc, block_idx):
        dk_acc, dv_acc = grad_acc
        row_start = block_idx * TOK_DEV
        q_blk = lax.dynamic_slice_in_dim(q_all, row_start, TOK_DEV, 0).astype(jnp.float32)
        do_blk = lax.dynamic_slice_in_dim(do_all, row_start, TOK_DEV, 0).astype(jnp.float32)
        pos_blk = lax.dynamic_slice_in_dim(all_pos, row_start, TOK_DEV, 0)
        doc_blk = lax.dynamic_slice_in_dim(doc_id, row_start, TOK_DEV, 0)
        visible = (all_pos[None, :] <= pos_blk[:, None]) & (doc_id[None, :] == doc_blk[:, None])
        scores = jnp.einsum('tkge,ske->tkgs', q_blk, k_wide) * score_scale
        scores = jnp.where(visible[:, None, None, :], scores, NEG_BIG)
        log_norm = jax.nn.logsumexp(scores, axis=-1, keepdims=True)
        prob_blk = jnp.exp(scores - log_norm).astype(jnp.bfloat16).astype(jnp.float32)
        out_blk = jnp.einsum('tkgs,ske->tkge', prob_blk, v_wide).astype(jnp.bfloat16).astype(jnp.float32)
        delta_row = jnp.sum(do_blk * out_blk, axis=-1, keepdims=True)
        d_prob = jnp.einsum('tkge,ske->tkgs', do_blk, v_wide)
        d_score = (prob_blk * (d_prob - delta_row)).astype(jnp.bfloat16).astype(jnp.float32)
        dq_blk = (jnp.einsum('tkgs,ske->tkge', d_score, k_wide) * score_scale).astype(jnp.bfloat16)
        dk_acc = dk_acc + jnp.einsum('tkgs,tkge->ske', d_score, q_blk) * score_scale
        dv_acc = dv_acc + jnp.einsum('tkgs,tkge->ske', prob_blk, do_blk)
        return (dk_acc, dv_acc), (out_blk.astype(jnp.bfloat16), dq_blk)

    zero_grad = jnp.zeros((SEQ_LEN, KV_HEADS, HEAD_DIM), jnp.float32)
    grad_sums, block_outs = lax.scan(block_step, (zero_grad, zero_grad), jnp.arange(GROUP_DEVS))
    dk_sum, dv_sum = grad_sums
    out_blocks, dq_blocks = block_outs
    out_all = out_blocks.reshape(SEQ_LEN, Q_HEADS * HEAD_DIM)
    dq_all = dq_blocks.reshape(SEQ_LEN, Q_HEADS * HEAD_DIM)
    y_out = jnp.dot(out_all, wo_flat, preferred_element_type=jnp.float32).astype(jnp.bfloat16)
    dk_bf = dk_sum.astype(jnp.bfloat16).reshape(SEQ_LEN, KV_HEADS * HEAD_DIM)
    dv_bf = dv_sum.astype(jnp.bfloat16).reshape(SEQ_LEN, KV_HEADS * HEAD_DIM)
    dx_wide = (jnp.dot(dq_all, wq_flat.T, preferred_element_type=jnp.float32)
               + jnp.dot(dk_bf, wk_flat.T, preferred_element_type=jnp.float32)
               + jnp.dot(dv_bf, wv_flat.T, preferred_element_type=jnp.float32))
    dx_out = dx_wide.astype(jnp.bfloat16)
    return y_out, dx_out
```

```python
import functools
import math

import jax
import jax.numpy as jnp
from jax import lax
from jax.experimental import pallas as pl
from jax.experimental.pallas import tpu as pltpu
from jax.sharding import PartitionSpec as P

NEG_BIG = -1.0e30
MESH = pl.DeviceIdType.MESH
VMEM = pltpu.VMEM
F32 = jnp.float32
BF16 = jnp.bfloat16


def remote(src, dst, send_sem, recv_sem, dev):
    return pltpu.make_async_remote_copy(src_ref=src, dst_ref=dst, send_sem=send_sem, recv_sem=recv_sem,
                                        device_id={'cp': dev}, device_id_type=MESH)


def small_gather_kernel(n, x_ref, out_ref, send_sem, recv_sem, own_sem):
    me = lax.axis_index('cp')
    barrier = pltpu.get_barrier_semaphore()

    def greet(off, _):
        pl.semaphore_signal(barrier, inc=1, device_id={'cp': lax.rem(me + off, n)}, device_id_type=MESH)
        return 0
    lax.fori_loop(1, n, greet, 0)
    own = pltpu.make_async_copy(x_ref, out_ref.at[me], own_sem)
    own.start()
    pl.semaphore_wait(barrier, n - 1)

    def send(off, _):
        remote(x_ref, out_ref.at[me], send_sem.at[off], recv_sem.at[off], lax.rem(me + off, n)).start()
        return 0
    lax.fori_loop(1, n, send, 0)
    own.wait()

    def settle(off, _):
        src = lax.rem(me + n - off, n)
        copy = remote(x_ref, out_ref.at[src], send_sem.at[off], recv_sem.at[off], lax.rem(me + off, n))
        copy.wait_send()
        copy.wait_recv()
        return 0
    lax.fori_loop(1, n, settle, 0)


def small_gather(x, n, cid):
    return pl.pallas_call(
        functools.partial(small_gather_kernel, n),
        out_shape=jax.ShapeDtypeStruct((n,) + x.shape, x.dtype),
        in_specs=[pl.BlockSpec(memory_space=VMEM)],
        out_specs=pl.BlockSpec(memory_space=VMEM),
        scratch_shapes=[pltpu.SemaphoreType.DMA((n,)), pltpu.SemaphoreType.DMA((n,)), pltpu.SemaphoreType.DMA],
        compiler_params=pltpu.CompilerParams(collective_id=cid, has_side_effects=True),
        name=f'small_gather_{cid}',
    )(x)


def torus_gather_kernel(side, x_ref, out_ref, send_sem, recv_sem, chip_send, chip_recv, own_sem):
    me = lax.axis_index('cp')
    core = lax.rem(me, 2)
    chip = me // 2
    cx, cy = lax.rem(chip, side), chip // side

    def dev(y, x, c=None):
        y = lax.rem(cy + y + side, side)
        x = lax.rem(cx + x + side, side)
        return (y * side + x) * 2 + (core if c is None else c)

    partner = dev(0, 0, 1 - core)
    barrier = pltpu.get_barrier_semaphore()
    for peer in (dev(0, 1), dev(0, -1), dev(1, 0), dev(-1, 0), partner):
        pl.semaphore_signal(barrier, inc=1, device_id={'cp': peer}, device_id_type=MESH)
    own = pltpu.make_async_copy(x_ref, out_ref.at[me], own_sem)
    own.start()
    pl.semaphore_wait(barrier, 5)

    sends = []

    def at(half, minor, major):
        return dev(major, minor) if half == 0 else dev(minor, major)

    def step(half, axis, amount):
        first = half == axis
        del first
        return at(half, amount, 0) if axis == 0 else at(half, 0, amount)

    slots = [0]
    plan = {}

    def slot(key):
        if key not in plan:
            plan[key] = len(plan)
        return plan[key]

    def ref_of(ref, d, half, ud):
        return ref.at[d, half] if ud is None else ref.at[d, half, ud]

    def send(half, axis, direction, minor, major, ud, own_block):
        d = at(half, minor, major)
        key = slot((half, axis, direction, minor, major, ud))
        src = (x_ref.at[half] if ud is None else x_ref.at[half, ud]) if own_block else ref_of(out_ref, d, half, ud)
        copy = remote(src, ref_of(out_ref, d, half, ud), send_sem.at[key], recv_sem.at[key], step(half, axis, direction))
        copy.start()
        sends.append(copy)

    def receive(half, axis, direction, minor, major, ud):
        key = slot((half, axis, direction, minor, major, ud))
        if axis == 0:
            my_minor, my_major = minor - direction, major
        else:
            my_minor, my_major = minor, major - direction
        d = at(half, my_minor, my_major)
        ref = ref_of(out_ref, d, half, ud)
        remote(ref, ref, send_sem.at[key], recv_sem.at[key], step(half, axis, direction)).wait_recv()
        return my_minor, my_major

    chip_count = [0]
    chip_waits = []

    def to_partner(half, minor, major, ud, own_block=False):
        d = at(half, minor, major)
        k = chip_count[0]
        chip_count[0] += 1
        src = (x_ref.at[half]) if own_block else ref_of(out_ref, d, half, ud)
        copy = remote(src, ref_of(out_ref, d, half, ud), chip_send.at[k], chip_recv.at[k], partner)
        copy.start()
        sends.append(copy)
        chip_waits.append((half, minor, major, ud, k))

    for half in (0, 1):
        for direction in (1, -1):
            send(half, 0, direction, 0, 0, None, True)
    for half in (0, 1):
        for direction in (1, -1):
            send(half, 1, direction, 0, 0, None, True)
        to_partner(half, 0, 0, None, True)

    for direction in (1, -1):
        for half in (0, 1):
            minor, major = receive(half, 0, direction, 0, 0, None)
            ud = 0 if direction == 1 else 1
            send(half, 0, direction, minor, major, ud, False)
            for way in (1, -1):
                send(half, 1, way, minor, major, None, False)
            to_partner(half, minor, major, None)
    for direction in (1, -1):
        for half in (0, 1):
            ud = 0 if direction == 1 else 1
            minor, major = receive(half, 0, direction, -direction, 0, ud)
            for way in (1, -1):
                send(half, 1, way, minor, major, ud, False)
            to_partner(half, minor, major, ud)
    for minor in (0, -1, 1):
        for direction in (1, -1):
            for half in (0, 1):
                _, major = receive(half, 1, direction, minor, 0, None)
                ud = 0 if direction == 1 else 1
                send(half, 1, direction, minor, major, ud, False)
                to_partner(half, minor, major, None)
    for ud, minor in ((0, -2), (1, 2)):
        for direction in (1, -1):
            for half in (0, 1):
                _, major = receive(half, 1, direction, minor, 0, ud)
                if ud == (0 if direction == 1 else 1):
                    send(half, 1, direction, minor, major, ud, False)
                to_partner(half, minor, major, ud)
    for minor in (0, -1, 1):
        for direction in (1, -1):
            for half in (0, 1):
                ud = 0 if direction == 1 else 1
                _, major = receive(half, 1, direction, minor, -direction, ud)
                to_partner(half, minor, major, ud)
    for ud, minor in ((0, -2), (1, 2)):
        for half in (0, 1):
            direction = 1 if ud == 0 else -1
            _, major = receive(half, 1, direction, minor, -direction, ud)
            to_partner(half, minor, major, ud)
    for half, minor, major, ud, k in chip_waits:
        base = at(half, minor, major)
        d = base + 1 - 2 * core
        ref = ref_of(out_ref, d, half, ud)
        remote(ref, ref, chip_send.at[k], chip_recv.at[k], partner).wait_recv()
    for copy in sends:
        copy.wait_send()
    own.wait()


def torus_gather(x, n, cid):
    side = math.isqrt(n // 2)
    return pl.pallas_call(
        functools.partial(torus_gather_kernel, side),
        out_shape=jax.ShapeDtypeStruct((n,) + x.shape, x.dtype),
        in_specs=[pl.BlockSpec(memory_space=VMEM)],
        out_specs=pl.BlockSpec(memory_space=pltpu.HBM),
        scratch_shapes=[pltpu.SemaphoreType.DMA((64,)), pltpu.SemaphoreType.DMA((64,)),
                        pltpu.SemaphoreType.DMA((64,)), pltpu.SemaphoreType.DMA((64,)), pltpu.SemaphoreType.DMA],
        compiler_params=pltpu.CompilerParams(collective_id=cid, has_side_effects=True),
        name='torus_gather',
    )(x)


def dot_nt(a, b):
    return lax.dot_general(a, b, (((1,), (1,)), ((), ())), preferred_element_type=F32)


def dot_nn(a, b):
    return lax.dot_general(a, b, (((1,), (0,)), ((), ())), preferred_element_type=F32)


def query_kernel(pieces, plen, hd, scale, meta, a_ref, start_ref, g_ref, o_ref, dq_ref, ld_ref, kv, p_s, q2, do2, sem):
    half_rows = plen // 2
    for t in range(2):
        c, lo = meta[t], meta[2 + t]
        count = c - lo + 1

        def fetch(i):
            p = lo + i
            far = (p >= pieces // 2).astype(jnp.int32)
            d = jnp.where(far == 1, pieces - 1 - p, p)
            return [pltpu.make_async_copy(g_ref.at[d, h, far, :, pl.ds(0, 2 * hd)], kv.at[i, pl.ds(h * half_rows, half_rows)],
                                          sem.at[h, i]) for h in range(2)]

        def issue(i, _):
            for copy in fetch(i):
                copy.start()
            return 0
        lax.fori_loop(0, count, issue, 0)
        for h in range(2):
            for part in range(2):
                rows = pl.ds(h * plen + part * half_rows, half_rows)
                q2[rows, :] = a_ref[part, t, :, pl.ds((2 + h) * hd, hd)]
                do2[rows, :] = a_ref[part, t, :, pl.ds((4 + h) * hd, hd)]
        first = start_ref[t]
        first = jnp.concatenate([first, first], axis=0)
        row = lax.broadcasted_iota(jnp.int32, (plen, 1), 0) + c * plen
        row = jnp.concatenate([row, row], axis=0)

        def scores(i):
            s = dot_nt(q2[...], kv[i, :, pl.ds(0, hd)]) * scale
            col = lax.broadcasted_iota(jnp.int32, (1, plen), 1) + (lo + i) * plen
            return jnp.where((col >= first) & (col <= row), s, NEG_BIG)

        def sweep_norm(i, carry):
            m, l = carry
            for copy in fetch(i):
                copy.wait()
            s = scores(i)
            parts = [s[:, k:k + 128] for k in range(0, plen, 128)]
            m_new = m
            for part in parts:
                m_new = jnp.maximum(m_new, part)
            l = l * jnp.exp(m - m_new)
            for part in parts:
                l = l + jnp.exp(part - m_new)
            return m_new, l
        m, l = lax.fori_loop(0, count, sweep_norm,
                             (jnp.full((2 * plen, 128), NEG_BIG, F32), jnp.zeros((2 * plen, 128), F32)))
        top = jnp.max(m, axis=1, keepdims=True)
        total = jnp.sum(l * jnp.exp(m - top), axis=1, keepdims=True)
        log_norm = top + jnp.log(total)

        def sweep_out(i, acc):
            p = jnp.exp(scores(i) - log_norm).astype(BF16)
            p_s[i] = p
            return acc + dot_nn(p, kv[i, :, pl.ds(hd, hd)])
        out = lax.fori_loop(0, count, sweep_out, jnp.zeros((2 * plen, hd), F32)).astype(BF16)
        delta = jnp.sum(do2[...].astype(F32) * out.astype(F32), axis=1, keepdims=True)

        def sweep_dq(i, acc):
            dp = dot_nt(do2[...], kv[i, :, pl.ds(hd, hd)])
            ds = (p_s[i].astype(F32) * (dp - delta)).astype(BF16)
            return acc + dot_nn(ds, kv[i, :, pl.ds(0, hd)])
        dq = (lax.fori_loop(0, count, sweep_dq, jnp.zeros((2 * plen, hd), F32)) * scale).astype(BF16)
        for h in range(2):
            o_ref[pl.ds(t * plen, plen), pl.ds(h * hd, hd)] = out[h * plen:(h + 1) * plen]
            dq_ref[pl.ds(t * plen, plen), pl.ds(h * hd, hd)] = dq[h * plen:(h + 1) * plen]
        lrow = jnp.transpose(jnp.broadcast_to(log_norm, (2 * plen, 128)))
        drow = jnp.transpose(jnp.broadcast_to(delta, (2 * plen, 128)))
        for h in range(2):
            ld_ref[pl.ds(4 * t + h, 1), :] = lrow[0:1, h * plen:(h + 1) * plen]
            ld_ref[pl.ds(4 * t + 2 + h, 1), :] = drow[0:1, h * plen:(h + 1) * plen]


def key_kernel(pieces, plen, hd, scale, meta, a_ref, end_ref, ld_ref, g_ref, dk_ref, dv_ref, qd, kt, vt, dk_acc, dv_acc, sem):
    half_rows = plen // 2
    for t in range(2):
        c, hi = meta[t], meta[4 + t]
        count = hi - c + 1

        def fetch(i):
            p = c + i
            far = (p >= pieces // 2).astype(jnp.int32)
            d = jnp.where(far == 1, pieces - 1 - p, p)
            b = lax.rem(i, 2)
            return [pltpu.make_async_copy(g_ref.at[d, h, far, :, pl.ds(2 * hd, 4 * hd)],
                                          qd.at[b, pl.ds(h * half_rows, half_rows)], sem.at[b, h]) for h in range(2)]

        for copy in fetch(0):
            copy.start()
        for part in range(2):
            rows = pl.ds(part * half_rows, half_rows)
            kt[rows, :] = a_ref[part, t, :, pl.ds(0, hd)]
            vt[rows, :] = a_ref[part, t, :, pl.ds(hd, hd)]
        dk_acc[...] = jnp.zeros_like(dk_acc)
        dv_acc[...] = jnp.zeros_like(dv_acc)
        last = end_ref[t]
        key = lax.broadcasted_iota(jnp.int32, (plen, 1), 0) + c * plen

        def sweep(i, _):
            @pl.when(i + 1 < count)
            def _():
                for copy in fetch(i + 1):
                    copy.start()
            for copy in fetch(i):
                copy.wait()
            b = lax.rem(i, 2)
            p_idx = c + i
            far = (p_idx >= pieces // 2).astype(jnp.int32)
            d = jnp.where(far == 1, pieces - 1 - p_idx, p_idx)
            col = lax.broadcasted_iota(jnp.int32, (1, plen), 1) + p_idx * plen
            seen = (col >= key) & (col <= last)
            for h in range(2):
                qh = qd[b, :, pl.ds(h * hd, hd)]
                doh = qd[b, :, pl.ds((2 + h) * hd, hd)]
                st = dot_nt(kt[...], qh) * scale
                st = jnp.where(seen, st, NEG_BIG)
                norm = ld_ref[d, pl.ds(4 * far + h, 1), :]
                delta = ld_ref[d, pl.ds(4 * far + 2 + h, 1), :]
                pt = jnp.exp(st - norm).astype(BF16)
                dv_acc[...] += dot_nn(pt, doh)
                dpt = dot_nt(vt[...], doh)
                dst = (pt.astype(F32) * (dpt - delta)).astype(BF16)
                dk_acc[...] += dot_nn(dst, qh)
            return 0
        lax.fori_loop(0, count, sweep, 0)
        dk_ref[pl.ds(t * plen, plen), :] = (dk_acc[...] * scale).astype(BF16)
        dv_ref[pl.ds(t * plen, plen), :] = dv_acc[...].astype(BF16)


def solution(mesh):
    n = mesh.shape['cp']
    row_spec = P(('dp', 'cp'))
    full_spec = P()

    def local_layer(x_in, dy_in, doc_id, w_q, w_k, w_v, w_o):
        tok, d_model = x_in.shape
        heads, hd = w_q.shape[1], w_q.shape[2]
        plen = tok // 2
        pieces = 2 * n
        seq = tok * n
        scale = hd ** -0.5
        me = lax.axis_index('cp')
        wq = w_q.reshape(d_model, heads * hd)
        wk = w_k.reshape(d_model, hd)
        wv = w_v.reshape(d_model, hd)
        wo = w_o.reshape(heads * hd, d_model)

        lane = 128
        doc_pad = jnp.zeros((8, lane), jnp.int32).at[:tok // lane].set(doc_id.reshape(tok // lane, lane))
        docs = small_gather(doc_pad, n, 1)[:, :tok // lane].reshape(n, 2, plen)
        doc_all = jnp.concatenate([docs[:, 0].reshape(-1), docs[::-1, 1].reshape(-1)])
        start = jnp.sum((doc_all[None, :] < doc_id[:, None]).astype(jnp.int32), axis=1)
        end = jnp.sum((doc_all[None, :] <= doc_id[:, None]).astype(jnp.int32), axis=1) - 1
        own = jnp.stack([me, pieces - 1 - me]).astype(jnp.int32)
        meta = jnp.concatenate([own, start[::plen] // plen, end[plen - 1::plen] // plen]).astype(jnp.int32)

        def mm(a, b):
            return jnp.dot(a, b, preferred_element_type=F32).astype(BF16)
        k_loc, v_loc, q_loc = mm(x_in, wk), mm(x_in, wv), mm(x_in, wq)
        do_loc = lax.dot_general(dy_in, wo, (((1,), (1,)), ((), ())), preferred_element_type=F32).astype(BF16)
        a_loc = jnp.concatenate([k_loc, v_loc, q_loc, do_loc], axis=1)
        width = a_loc.shape[1]
        a_loc = a_loc.reshape(2, 2, plen // 2, width).transpose(1, 0, 2, 3)
        g_all = torus_gather(a_loc, n, 2)

        smem = pl.BlockSpec(memory_space=pltpu.SMEM)
        vmem = pl.BlockSpec(memory_space=VMEM)
        hbm = pl.BlockSpec(memory_space=pltpu.HBM)
        o_loc, dq_loc, ld = pl.pallas_call(
            functools.partial(query_kernel, pieces, plen, hd, scale),
            out_shape=(jax.ShapeDtypeStruct((tok, heads * hd), BF16), jax.ShapeDtypeStruct((tok, heads * hd), BF16),
                       jax.ShapeDtypeStruct((8, plen), F32)),
            in_specs=[smem, vmem, vmem, hbm], out_specs=(vmem, vmem, vmem),
            scratch_shapes=[VMEM((pieces, plen, 2 * hd), BF16), VMEM((pieces, 2 * plen, plen), BF16),
                            VMEM((2 * plen, hd), BF16), VMEM((2 * plen, hd), BF16), pltpu.SemaphoreType.DMA((2, pieces))],
            compiler_params=pltpu.CompilerParams(vmem_limit_bytes=60 * 1024 * 1024),
            name='query_side',
        )(meta, a_loc, start.reshape(2, plen, 1), g_all)
        ld_all = small_gather(ld, n, 3)
        dk_loc, dv_loc = pl.pallas_call(
            functools.partial(key_kernel, pieces, plen, hd, scale),
            out_shape=(jax.ShapeDtypeStruct((tok, hd), BF16), jax.ShapeDtypeStruct((tok, hd), BF16)),
            in_specs=[smem, vmem, vmem, vmem, hbm], out_specs=(vmem, vmem),
            scratch_shapes=[VMEM((2, plen, 4 * hd), BF16), VMEM((plen, hd), BF16), VMEM((plen, hd), BF16),
                            VMEM((plen, hd), F32), VMEM((plen, hd), F32), pltpu.SemaphoreType.DMA((2, 2))],
            name='key_side',
        )(meta, a_loc, end.reshape(2, plen, 1), ld_all, g_all)
        y_out = mm(o_loc, wo)
        nt = (((1,), (1,)), ((), ()))
        dx = (lax.dot_general(dq_loc, wq, nt, preferred_element_type=F32)
              + lax.dot_general(dk_loc, wk, nt, preferred_element_type=F32)
              + lax.dot_general(dv_loc, wv, nt, preferred_element_type=F32))
        return y_out, dx.astype(BF16)

    return jax.shard_map(local_layer, mesh=mesh,
                         in_specs=(row_spec, row_spec, row_spec, full_spec, full_spec, full_spec, full_spec),
                         out_specs=(row_spec, row_spec), check_vma=False)
```

```python
import collections
import functools
import heapq
import math
import random

import jax
import jax.numpy as jnp
from jax import lax
from jax.experimental import pallas as pl
from jax.experimental.pallas import tpu as pltpu
from jax.sharding import PartitionSpec as P

NEG_BIG = -1.0e30
MESH = pl.DeviceIdType.MESH
VMEM = pltpu.VMEM
F32 = jnp.float32
REACHES = (11, 13, 16, 20)
TUNES = ((1.2, 3.0, 29), (1.05, 0.3, 30), (1.2, 3.0, 49), (1.05, 1.0, 15), (1.05, 0.3, 52))
PARTS = 2
BF16 = jnp.bfloat16


def remote(src, dst, send_sem, recv_sem, dev):
    return pltpu.make_async_remote_copy(src_ref=src, dst_ref=dst, send_sem=send_sem, recv_sem=recv_sem,
                                        device_id={'cp': dev}, device_id_type=MESH)


def small_gather_kernel(n, x_ref, out_ref, send_sem, recv_sem, own_sem):
    me = lax.axis_index('cp')
    barrier = pltpu.get_barrier_semaphore()

    def greet(off, _):
        pl.semaphore_signal(barrier, inc=1, device_id={'cp': lax.rem(me + off, n)}, device_id_type=MESH)
        return 0
    lax.fori_loop(1, n, greet, 0)
    own = pltpu.make_async_copy(x_ref, out_ref.at[me], own_sem)
    own.start()
    pl.semaphore_wait(barrier, n - 1)

    def send(off, _):
        remote(x_ref, out_ref.at[me], send_sem.at[off], recv_sem.at[off], lax.rem(me + off, n)).start()
        return 0
    lax.fori_loop(1, n, send, 0)
    own.wait()

    def settle(off, _):
        src = lax.rem(me + n - off, n)
        copy = remote(x_ref, out_ref.at[src], send_sem.at[off], recv_sem.at[off], lax.rem(me + off, n))
        copy.wait_send()
        copy.wait_recv()
        return 0
    lax.fori_loop(1, n, settle, 0)


def small_gather(x, n, cid):
    return pl.pallas_call(
        functools.partial(small_gather_kernel, n),
        out_shape=jax.ShapeDtypeStruct((n,) + x.shape, x.dtype),
        in_specs=[pl.BlockSpec(memory_space=VMEM)],
        out_specs=pl.BlockSpec(memory_space=VMEM),
        scratch_shapes=[pltpu.SemaphoreType.DMA((n,)), pltpu.SemaphoreType.DMA((n,)), pltpu.SemaphoreType.DMA],
        compiler_params=pltpu.CompilerParams(collective_id=cid, has_side_effects=True),
        name=f'small_gather_{cid}',
    )(x)


def needs(side, reach):
    chips = side * side
    last = 4 * chips - 1
    out = {}
    for dev in range(2 * chips):
        for s in (0, 1):
            kv, qd = (dev, last - dev) if s == 0 else (last - dev, dev)
            out[dev, s] = {k for k in range(chips) for c in (2 * k, 2 * k + 1, last - 2 * k, last - 2 * k - 1)
                           if k != dev // 2 and (0 < c - kv <= reach or 0 < qd - c <= reach)}
    return out


def neighbours(side, chip):
    x, y = chip % side, chip // side
    return ((y * side + (x + 1) % side, 0), (y * side + (x - 1) % side, 1),
            ((y + 1) % side * side + x, 2), ((y - 1) % side * side + x, 3))


def grow(side, load, src, targets, steep, hop):
    depth = {src: 0}
    edges = []
    missing = set(targets)
    while missing:
        dist = {c: depth[c] * hop for c in depth}
        back = {}
        heap = sorted((d, c) for c, d in dist.items())
        done = set()
        while True:
            d, c = heapq.heappop(heap)
            if c in done:
                continue
            done.add(c)
            if c in missing:
                break
            for nb, way in neighbours(side, c):
                w = d + steep ** load[c, way] + hop
                if nb not in depth and w < dist.get(nb, 1e30):
                    dist[nb], back[nb] = w, (c, way)
                    heapq.heappush(heap, (w, nb))
        path = []
        while c not in depth:
            path.append((back[c][0], back[c][1], c))
            c = back[c][0]
        for p, way, c in reversed(path):
            depth[c] = depth[p] + 1
            edges.append((p, way, c))
            missing.discard(c)
    return edges, depth


def unit_key(side, depth, src, chip, s, h):
    return depth, (src // side - chip // side) % side, (src % side - chip % side) % side, s, h


def arrivals(side, trees, order, hold, lag):
    todo = collections.defaultdict(list)
    for (dev, s, h), (edges, depth) in trees.items():
        onward = collections.defaultdict(list)
        for p, way, c in edges:
            onward[p].append((way, c))
        for c in depth:
            key = unit_key(side, depth[c], dev // 2, c, s, h)
            todo[c, dev % 2].append((order(key), key, (dev, s, h), onward[c]))
    came = {(dev // 2, (dev, s, h)): 0.0 for dev, s, h in trees}
    clock, free, seen = collections.Counter(), collections.Counter(), collections.defaultdict(list)
    queues = {place: sorted(v, key=lambda u: u[:2], reverse=True) for place, v in todo.items()}
    moved = True
    while moved:
        moved = False
        for place, queue in queues.items():
            while queue and (place[0], queue[-1][2]) in came:
                _, key, unit, onward = queue.pop()
                clock[place] = max(clock[place], came[place[0], unit])
                seen[key].append(came[place[0], unit])
                for way, c in onward:
                    free[place, way] = max(clock[place], free[place, way]) + hold
                    came[c, unit] = free[place, way] + lag
                moved = True
    return max(came.values()), {k: sum(v) / len(v) for k, v in seen.items()}


def plan(side, reach, parts, tune):
    steep, hop, seed = tune
    nd = needs(side, reach)
    keys = [(dev, s, h) for h in range(parts) for dev in range(2 * side * side) for s in (0, 1)]
    random.Random(seed).shuffle(keys)
    load, trees, best = collections.Counter(), {}, None
    for _ in range(6):
        for key in keys:
            for p, way, c in trees.get(key, ((), ()))[0]:
                load[p, way] -= 1
            trees[key] = grow(side, load, key[0] // 2, nd[key[0], key[1]], steep, hop)
            for p, way, c in trees[key][0]:
                load[p, way] += 1
        mean = {}
        for _ in range(5):
            end, later = arrivals(side, trees, lambda k: (k[0], round(mean.get(k, 0.0), 3)), 16.9 / parts, 2.5)
            if best is None or end < best[0]:
                best = end, dict(trees), mean
            mean = later
    units = collections.defaultdict(lambda: dict(take=0, send=[0] * 4, keep=0, given=0))
    for (dev, s, h), (edges, depth) in best[1].items():
        src, core = dev // 2, dev % 2

        def unit(c):
            return units[unit_key(side, depth[c], src, c, s, h)]
        for p, way, c in edges:
            unit(c)['take'] |= 1 << (2 * c + core)
            unit(p)['send'][way] |= 1 << (2 * p + core)
        for c in nd[dev, s] | {src}:
            unit(c)['keep'] |= 1 << (2 * c + core)
            unit(c)['given'] |= 1 << (2 * c + 1 - core)
    order = sorted(units.items(), key=lambda kv: (kv[0][0], round(best[2].get(kv[0], 0.0), 3), kv[0]))
    return [(k, v['take'], v['send'], v['keep'], v['given']) for k, v in order]


def multicast_kernel(side, parts, units, x_ref, out_ref, send_sem, recv_sem, chip_send, chip_recv, own_sem):
    me = lax.axis_index('cp')
    core = lax.rem(me, 2)
    chip = me // 2
    cx, cy = lax.rem(chip, side), chip // side
    rows = x_ref.shape[1] // parts
    bit = lax.shift_left(jnp.int32(1), me.astype(jnp.int32))

    def among(mask):
        mask = mask - (1 << 32) if mask >> 31 else mask
        return (bit & jnp.int32(mask)) != 0

    def dev(y, x, c):
        return (lax.rem(cy + y + side, side) * side + lax.rem(cx + x + side, side)) * 2 + c

    partner = dev(0, 0, 1 - core)
    ways = (dev(0, 1, core), dev(0, -1, core), dev(1, 0, core), dev(-1, 0, core))
    barrier = pltpu.get_barrier_semaphore()
    for peer in ways + (partner,):
        pl.semaphore_signal(barrier, inc=1, device_id={'cp': peer}, device_id_type=MESH)
    own = pltpu.make_async_copy(x_ref, out_ref.at[me], own_sem)
    own.start()
    pl.semaphore_wait(barrier, 5)

    sends = []
    slot = {key: k for k, (key, *_) in enumerate(units)}
    for k, ((depth, dy, dx, s, h), take, send, keep, given) in enumerate(units):
        mine = dy == 0 and dx == 0
        block = pl.ds(h * rows, rows)
        here = out_ref.at[dev(dy, dx, core), s, block]
        src = x_ref.at[s, block] if mine else here

        def push():
            for way, mask in enumerate(send):
                if mask:
                    ahead = (dy - (0, 0, 1, -1)[way]) % side, (dx - (1, -1, 0, 0)[way]) % side
                    copy = remote(src, here, send_sem.at[len(sends)], recv_sem.at[slot[depth + 1, *ahead, s, h]], ways[way])
                    sends.append((mask, copy))
                    pl.when(among(mask))(copy.start)
            if keep:
                copy = remote(src, here, chip_send.at[k], chip_recv.at[k], partner)
                sends.append((keep, copy))
                pl.when(among(keep))(copy.start)
        if take:
            pl.when(among(take))(remote(here, here, send_sem.at[0], recv_sem.at[k], partner).wait_recv)
        push()
    for k, ((_, dy, dx, s, h), take, send, keep, given) in enumerate(units):
        there = out_ref.at[dev(dy, dx, 1 - core), s, pl.ds(h * rows, rows)]
        if given:
            pl.when(among(given))(remote(there, there, chip_send.at[k], chip_recv.at[k], partner).wait_recv)
    for mask, copy in sends:
        pl.when(among(mask))(copy.wait_send)
    own.wait()


def multicast(x, n, reach, tune, parts, cid):
    side = math.isqrt(n // 2)
    units = plan(side, reach, parts, tune)
    count = sum(1 for u in units for m in u[2] if m) + len(units)
    sems = [pltpu.SemaphoreType.DMA((c,)) for c in (count, len(units), len(units), len(units))]
    return pl.pallas_call(
        functools.partial(multicast_kernel, side, parts, units),
        out_shape=jax.ShapeDtypeStruct((n,) + x.shape, x.dtype),
        in_specs=[pl.BlockSpec(memory_space=VMEM)],
        out_specs=pl.BlockSpec(memory_space=pltpu.HBM),
        scratch_shapes=sems + [pltpu.SemaphoreType.DMA],
        compiler_params=pltpu.CompilerParams(collective_id=cid, has_side_effects=True),
        name=f'multicast_{reach}',
    )(x)


def dot_nt(a, b):
    return lax.dot_general(a, b, (((1,), (1,)), ((), ())), preferred_element_type=F32)


def dot_nn(a, b):
    return lax.dot_general(a, b, (((1,), (0,)), ((), ())), preferred_element_type=F32)


def query_kernel(pieces, plen, hd, scale, meta, a_ref, docs_ref, mine_ref, g_ref, o_ref, dq_ref, ld_ref,
                 kv, p_s, q2, do2, m_s, l_s, acc, sem):
    wide = 2 * plen
    for t in range(2):
        c, lo = meta[t], meta[2 + t]
        blocks = (c - lo + 2) // 2

        def fetch(i):
            p = jnp.minimum(lo + i, c)
            far = (p >= pieces // 2).astype(jnp.int32)
            d = jnp.where(far == 1, pieces - 1 - p, p)
            return pltpu.make_async_copy(g_ref.at[d, far, :, pl.ds(0, 2 * hd)], kv.at[pl.ds(i * plen, plen)], sem.at[i])

        def issue(i, _):
            fetch(i).start()
            return 0
        lax.fori_loop(0, 2 * blocks, issue, 0)
        for h in range(2):
            rows = pl.ds(h * plen, plen)
            q2[rows, :] = a_ref[1 - t, :, pl.ds((2 + h) * hd, hd)]
            do2[rows, :] = a_ref[1 - t, :, pl.ds((4 + h) * hd, hd)]
        m_s[...] = jnp.full_like(m_s, NEG_BIG)
        l_s[...] = jnp.zeros_like(l_s)
        acc[...] = jnp.zeros_like(acc)
        doc = mine_ref[t]
        doc = jnp.concatenate([doc, doc], axis=0)
        row = lax.broadcasted_iota(jnp.int32, (plen, 1), 0) + c * plen
        row = jnp.concatenate([row, row], axis=0)

        def keys(i):
            return pl.ds(pl.multiple_of(i * wide, wide), wide)

        def scores(i):
            s = dot_nt(q2[...], kv[keys(i), pl.ds(0, hd)]) * scale
            p = lo + 2 * i
            key_doc = jnp.concatenate([docs_ref[pl.ds(p, 1), :], docs_ref[pl.ds(jnp.minimum(p + 1, c), 1), :]], axis=1)
            col = lax.broadcasted_iota(jnp.int32, (1, wide), 1) + p * plen
            return jnp.where((key_doc == doc) & (col <= row), s, NEG_BIG)

        def sweep_norm(i, _):
            fetch(2 * i).wait()
            fetch(2 * i + 1).wait()
            s = scores(i)
            parts = [s[:, k:k + 128] for k in range(0, wide, 128)]
            m = m_s[...]
            m_new = jnp.maximum(m, functools.reduce(jnp.maximum, parts))
            l_s[...] = l_s[...] * jnp.exp(m - m_new) + sum(jnp.exp(part - m_new) for part in parts)
            m_s[...] = m_new
            return 0
        lax.fori_loop(0, blocks, sweep_norm, 0)
        top = jnp.max(m_s[...], axis=1, keepdims=True)
        total = jnp.sum(l_s[...] * jnp.exp(m_s[...] - top), axis=1, keepdims=True)
        log_norm = top + jnp.log(total)

        def sweep_out(i, _):
            p = jnp.exp(scores(i) - log_norm).astype(BF16)
            p_s[i] = p
            acc[...] += dot_nn(p, kv[keys(i), pl.ds(hd, hd)])
            return 0
        lax.fori_loop(0, blocks, sweep_out, 0)
        out = acc[...].astype(BF16)
        delta = jnp.sum(do2[...].astype(F32) * out.astype(F32), axis=1, keepdims=True)
        acc[...] = jnp.zeros_like(acc)

        def sweep_dq(i, _):
            dp = dot_nt(do2[...], kv[keys(i), pl.ds(hd, hd)])
            ds = (p_s[i].astype(F32) * (dp - delta)).astype(BF16)
            acc[...] += dot_nn(ds, kv[keys(i), pl.ds(0, hd)])
            return 0
        lax.fori_loop(0, blocks, sweep_dq, 0)
        dq = (acc[...] * scale).astype(BF16)
        for h in range(2):
            o_ref[pl.ds(t * plen, plen), pl.ds(h * hd, hd)] = out[h * plen:(h + 1) * plen]
            dq_ref[pl.ds(t * plen, plen), pl.ds(h * hd, hd)] = dq[h * plen:(h + 1) * plen]
        ld_ref[pl.ds(2 * t, 1), :] = jnp.transpose(jnp.broadcast_to(log_norm, (wide, 128)))[0:1]
        ld_ref[pl.ds(2 * t + 1, 1), :] = jnp.transpose(jnp.broadcast_to(delta, (wide, 128)))[0:1]


def key_kernel(pieces, plen, hd, scale, meta, a_ref, docs_ref, mine_ref, ld_ref, g_ref, dk_ref, dv_ref,
               qd, kt, vt, dk_acc, dv_acc, sem):
    for t in range(2):
        c, hi = meta[t], meta[4 + t]
        count = hi - c + 1

        def place(i):
            p = c + i
            far = (p >= pieces // 2).astype(jnp.int32)
            return p, far, jnp.where(far == 1, pieces - 1 - p, p)

        def fetch(i):
            _, far, d = place(i)
            b = lax.rem(i, 3)
            return [pltpu.make_async_copy(g_ref.at[d, 1 - far, :, pl.ds((2 + k) * hd, hd)],
                                          qd.at[b, k // 2, pl.ds((k % 2) * plen, plen)], sem.at[b, k]) for k in range(4)]

        def start(i):
            for copy in fetch(i):
                copy.start()

        start(0)
        pl.when(count > 1)(lambda: start(1))
        kt[...] = a_ref[t, :, pl.ds(0, hd)]
        vt[...] = a_ref[t, :, pl.ds(hd, hd)]
        dk_acc[...] = jnp.zeros_like(dk_acc)
        dv_acc[...] = jnp.zeros_like(dv_acc)
        doc = mine_ref[t]
        key = lax.broadcasted_iota(jnp.int32, (plen, 1), 0)

        def sweep(i, _):
            pl.when(i + 2 < count)(lambda: start(i + 2))
            for copy in fetch(i):
                copy.wait()
            b = lax.rem(i, 3)
            p_idx, far, d = place(i)
            col = lax.broadcasted_iota(jnp.int32, (1, plen), 1) + i * plen
            seen = (docs_ref[pl.ds(p_idx, 1), :] == doc) & (col >= key)
            seen = jnp.concatenate([seen, seen], axis=1)
            st = jnp.where(seen, dot_nt(kt[...], qd[b, 0]) * scale, NEG_BIG)
            dpt = dot_nt(vt[...], qd[b, 1])
            pt = jnp.exp(st - ld_ref[d, pl.ds(2 * far, 1), :]).astype(BF16)
            dst = (pt.astype(F32) * (dpt - ld_ref[d, pl.ds(2 * far + 1, 1), :])).astype(BF16)
            dv_acc[...] += dot_nn(pt, qd[b, 1])
            dk_acc[...] += dot_nn(dst, qd[b, 0])
            return 0
        lax.fori_loop(0, count, sweep, 0)
        dk_ref[pl.ds(t * plen, plen), :] = (dk_acc[...] * scale).astype(BF16)
        dv_ref[pl.ds(t * plen, plen), :] = dv_acc[...].astype(BF16)


def solution(mesh):
    n = mesh.shape['cp']
    row_spec = P(('dp', 'cp'))
    full_spec = P()

    def local_layer(x_in, dy_in, doc_id, w_q, w_k, w_v, w_o):
        tok, d_model = x_in.shape
        heads, hd = w_q.shape[1], w_q.shape[2]
        plen = tok // 2
        pieces = 2 * n
        seq = tok * n
        scale = hd ** -0.5
        me = lax.axis_index('cp')
        wq = w_q.reshape(d_model, heads * hd)
        wk = w_k.reshape(d_model, hd)
        wv = w_v.reshape(d_model, hd)
        wo = w_o.reshape(heads * hd, d_model)

        lane = 128
        doc_pad = jnp.zeros((8, lane), jnp.int32).at[:tok // lane].set(doc_id.reshape(tok // lane, lane))
        docs = small_gather(doc_pad, n, 1)[:, :tok // lane].reshape(n, 2, plen)
        docs = jnp.concatenate([docs[:, 0], docs[::-1, 1]])
        first, last = docs[:, 0], docs[:, plen - 1]
        begun = jnp.sum((last[None, :] < first[:, None]).astype(jnp.int32), axis=1)
        ended = jnp.sum((first[None, :] <= last[:, None]).astype(jnp.int32), axis=1) - 1
        own = jnp.stack([me, pieces - 1 - me]).astype(jnp.int32)
        meta = jnp.concatenate([own, begun[own], ended[own]])
        mine = doc_id.reshape(2, plen, 1)

        def mm(a, b):
            return jnp.dot(a, b, preferred_element_type=F32).astype(BF16)
        k_loc, v_loc, q_loc = mm(x_in, wk), mm(x_in, wv), mm(x_in, wq)
        do_loc = lax.dot_general(dy_in, wo, (((1,), (1,)), ((), ())), preferred_element_type=F32).astype(BF16)
        a_loc = jnp.concatenate([r.reshape(2, plen, -1) for r in (k_loc, v_loc)]
                                + [r.reshape(2, plen, -1)[::-1] for r in (q_loc, do_loc)], axis=2)
        span = jnp.max(jnp.arange(pieces) - begun)
        level = jnp.sum((span > jnp.array(REACHES)).astype(jnp.int32))
        g_all = lax.switch(level, [functools.partial(multicast, n=n, reach=r, tune=TUNES[i], parts=PARTS, cid=4 + i)
                                   for i, r in enumerate(REACHES + (pieces,))], a_loc)

        smem = pl.BlockSpec(memory_space=pltpu.SMEM)
        vmem = pl.BlockSpec(memory_space=VMEM)
        hbm = pl.BlockSpec(memory_space=pltpu.HBM)
        o_loc, dq_loc, ld = pl.pallas_call(
            functools.partial(query_kernel, pieces, plen, hd, scale),
            out_shape=(jax.ShapeDtypeStruct((tok, heads * hd), BF16), jax.ShapeDtypeStruct((tok, heads * hd), BF16),
                       jax.ShapeDtypeStruct((4, 2 * plen), F32)),
            in_specs=[smem, vmem, vmem, vmem, hbm], out_specs=(vmem, vmem, vmem),
            scratch_shapes=[VMEM((pieces * plen, 2 * hd), BF16), VMEM((n, 2 * plen, 2 * plen), BF16),
                            VMEM((2 * plen, hd), BF16), VMEM((2 * plen, hd), BF16), VMEM((2 * plen, 128), F32),
                            VMEM((2 * plen, 128), F32), VMEM((2 * plen, hd), F32), pltpu.SemaphoreType.DMA((pieces,))],
            compiler_params=pltpu.CompilerParams(vmem_limit_bytes=60 * 1024 * 1024),
            name='query_side',
        )(meta, a_loc, docs, mine, g_all)
        ld_all = small_gather(ld, n, 3)
        dk_loc, dv_loc = pl.pallas_call(
            functools.partial(key_kernel, pieces, plen, hd, scale),
            out_shape=(jax.ShapeDtypeStruct((tok, hd), BF16), jax.ShapeDtypeStruct((tok, hd), BF16)),
            in_specs=[smem, vmem, vmem, vmem, vmem, hbm], out_specs=(vmem, vmem),
            scratch_shapes=[VMEM((3, 2, 2 * plen, hd), BF16), VMEM((plen, hd), BF16), VMEM((plen, hd), BF16),
                            VMEM((plen, hd), F32), VMEM((plen, hd), F32), pltpu.SemaphoreType.DMA((3, 4))],
            name='key_side',
        )(meta, a_loc, docs, mine, ld_all, g_all)
        y_out = mm(o_loc, wo)
        nt = (((1,), (1,)), ((), ()))
        dx = (lax.dot_general(dq_loc, wq, nt, preferred_element_type=F32)
              + lax.dot_general(dk_loc, wk, nt, preferred_element_type=F32)
              + lax.dot_general(dv_loc, wv, nt, preferred_element_type=F32))
        return y_out, dx.astype(BF16)

    return jax.shard_map(local_layer, mesh=mesh,
                         in_specs=(row_spec, row_spec, row_spec, full_spec, full_spec, full_spec, full_spec),
                         out_specs=(row_spec, row_spec), check_vma=False)
```

```python
import collections
import functools
import heapq
import math
import random

import jax
import jax.numpy as jnp
from jax import lax
from jax.experimental import pallas as pl
from jax.experimental.pallas import tpu as pltpu
from jax.sharding import PartitionSpec as P

NEG_BIG = -1.0e30
MESH = pl.DeviceIdType.MESH
VMEM = pltpu.VMEM
F32 = jnp.float32
REACHES = (20, 16, 11)
TUNES = ((1.05, 0.3, 52), (1.05, 1.0, 15), (1.2, 3.0, 49), (1.2, 3.0, 29))
PARTS = 2
BF16 = jnp.bfloat16


def remote(src, dst, send_sem, recv_sem, dev):
    return pltpu.make_async_remote_copy(src_ref=src, dst_ref=dst, send_sem=send_sem, recv_sem=recv_sem,
                                        device_id={'cp': dev}, device_id_type=MESH)


def exchange_kernel(n, hd, ld_ref, o_ref, wo_ref, all_ref, y_ref, wo_v, y_v, load_sem, store_sem, send_sem, recv_sem, own_sem):
    me = lax.axis_index('cp')
    barrier = pltpu.get_barrier_semaphore()
    load = pltpu.make_async_copy(wo_ref, wo_v, load_sem)
    load.start()

    def greet(off, _):
        pl.semaphore_signal(barrier, inc=1, device_id={'cp': lax.rem(me + off, n)}, device_id_type=MESH)
        return 0
    lax.fori_loop(1, n, greet, 0)
    own = pltpu.make_async_copy(ld_ref, all_ref.at[me], own_sem)
    own.start()
    pl.semaphore_wait(barrier, n - 1)

    def send(off, _):
        remote(ld_ref, all_ref.at[me], send_sem.at[off], recv_sem.at[off], lax.rem(me + off, n)).start()
        return 0
    lax.fori_loop(1, n, send, 0)
    load.wait()
    cols = 2 * hd
    count = y_ref.shape[1] // cols

    def store(j):
        at = pl.ds(pl.multiple_of(j * cols, cols), cols)
        return pltpu.make_async_copy(y_v.at[:, at], y_ref.at[:, at], store_sem.at[j])

    def column(j, _):
        at = pl.ds(pl.multiple_of(j * cols, cols), cols)
        y_v[:, at] = dot_nn(o_ref[...], wo_v[:, at]).astype(BF16)
        store(j).start()
        return 0
    lax.fori_loop(0, count, column, 0)
    own.wait()

    def settle(off, _):
        src = lax.rem(me + n - off, n)
        copy = remote(ld_ref, all_ref.at[src], send_sem.at[off], recv_sem.at[off], lax.rem(me + off, n))
        copy.wait_send()
        copy.wait_recv()
        return 0
    lax.fori_loop(1, n, settle, 0)

    def stored(j, _):
        store(j).wait()
        return 0
    lax.fori_loop(0, count, stored, 0)


def exchange(ld, o, wo, n, hd, cid):
    tok, d_model = o.shape[0], wo.shape[1]
    vmem, hbm = pl.BlockSpec(memory_space=VMEM), pl.BlockSpec(memory_space=pltpu.HBM)
    dma = pltpu.SemaphoreType.DMA
    return pl.pallas_call(
        functools.partial(exchange_kernel, n, hd),
        out_shape=(jax.ShapeDtypeStruct((n,) + ld.shape, ld.dtype), jax.ShapeDtypeStruct((tok, d_model), BF16)),
        in_specs=[vmem, vmem, hbm], out_specs=(vmem, hbm),
        scratch_shapes=[VMEM(wo.shape, BF16), VMEM((tok, d_model), BF16), dma, dma((d_model // (2 * hd),)), dma((n,)), dma((n,)), dma],
        compiler_params=pltpu.CompilerParams(collective_id=cid, has_side_effects=True, vmem_limit_bytes=32 * 1024 * 1024),
        name='exchange',
    )(ld, o, wo)


def project_kernel(n, hd, doc_ref, x_ref, dy_ref, wk_ref, wv_ref, wq_ref, wo_ref, out_ref, docs_ref,
                   x_v, dy_v, kv_v, wq_v, wo_v, load_sem, send_sem, recv_sem, own_sem):
    me = lax.axis_index('cp')
    barrier = pltpu.get_barrier_semaphore()

    def greet(off, _):
        pl.semaphore_signal(barrier, inc=1, device_id={'cp': lax.rem(me + off, n)}, device_id_type=MESH)
        return 0
    lax.fori_loop(1, n, greet, 0)
    loads = [pltpu.make_async_copy(src, dst, load_sem.at[i]) for i, (src, dst) in enumerate(
        ((x_ref, x_v), (wk_ref, kv_v.at[0]), (wv_ref, kv_v.at[1]), (wq_ref, wq_v), (dy_ref, dy_v), (wo_ref, wo_v)))]
    for load in loads:
        load.start()
    own = pltpu.make_async_copy(doc_ref, docs_ref.at[me], own_sem)
    own.start()
    half = x_ref.shape[0] // 2

    def fill(kind, src, weights, dot, col):
        def rows(t, _):
            out_ref[jnp.abs(t - kind), :, pl.ds(col, hd)] = dot(src[pl.ds(t * half, half), :], weights).astype(BF16)
            return 0
        lax.fori_loop(0, 2, rows, 0)

    loads[0].wait()
    for i in range(2):
        loads[1 + i].wait()
        fill(0, x_v, kv_v[i], dot_nn, i * hd)
    pl.semaphore_wait(barrier, n - 1)

    def send(off, _):
        remote(doc_ref, docs_ref.at[me], send_sem.at[off], recv_sem.at[off], lax.rem(me + off, n)).start()
        return 0
    lax.fori_loop(1, n, send, 0)
    loads[3].wait()
    for h in range(2):
        fill(1, x_v, wq_v[:, pl.ds(h * hd, hd)], dot_nn, (2 + h) * hd)
    loads[4].wait()
    loads[5].wait()
    for h in range(2):
        fill(1, dy_v, wo_v[pl.ds(h * hd, hd), :], dot_nt, (4 + h) * hd)
    own.wait()

    def settle(off, _):
        src = lax.rem(me + n - off, n)
        copy = remote(doc_ref, docs_ref.at[src], send_sem.at[off], recv_sem.at[off], lax.rem(me + off, n))
        copy.wait_send()
        copy.wait_recv()
        return 0
    lax.fori_loop(1, n, settle, 0)


def project(doc, x, dy, wk, wv, wq, wo, n, cid):
    tok, d_model = x.shape
    hd = wk.shape[1]
    vmem, hbm = pl.BlockSpec(memory_space=VMEM), pl.BlockSpec(memory_space=pltpu.HBM)
    return pl.pallas_call(
        functools.partial(project_kernel, n, hd),
        out_shape=(jax.ShapeDtypeStruct((2, tok // 2, 6 * hd), BF16), jax.ShapeDtypeStruct((n,) + doc.shape, doc.dtype)),
        in_specs=[vmem] + [hbm] * 6, out_specs=(vmem, vmem),
        scratch_shapes=[VMEM((tok, d_model), BF16), VMEM((tok, d_model), BF16), VMEM((2, d_model, hd), BF16),
                        VMEM((d_model, 2 * hd), BF16), VMEM((2 * hd, d_model), BF16), pltpu.SemaphoreType.DMA((6,)),
                        pltpu.SemaphoreType.DMA((n,)), pltpu.SemaphoreType.DMA((n,)), pltpu.SemaphoreType.DMA],
        compiler_params=pltpu.CompilerParams(collective_id=cid, has_side_effects=True, vmem_limit_bytes=48 * 1024 * 1024),
        name='project',
    )(doc, x, dy, wk, wv, wq, wo)


def small_gather(x, n, cid):
    return pl.pallas_call(
        functools.partial(small_gather_kernel, n),
        out_shape=jax.ShapeDtypeStruct((n,) + x.shape, x.dtype),
        in_specs=[pl.BlockSpec(memory_space=VMEM)],
        out_specs=pl.BlockSpec(memory_space=VMEM),
        scratch_shapes=[pltpu.SemaphoreType.DMA((n,)), pltpu.SemaphoreType.DMA((n,)), pltpu.SemaphoreType.DMA],
        compiler_params=pltpu.CompilerParams(collective_id=cid, has_side_effects=True),
        name=f'small_gather_{cid}',
    )(x)


def needs(side, reach):
    chips = side * side
    last = 4 * chips - 1
    out = {}
    for dev in range(2 * chips):
        for s in (0, 1):
            kv, qd = (dev, last - dev) if s == 0 else (last - dev, dev)
            out[dev, s] = {k for k in range(chips) for c in (2 * k, 2 * k + 1, last - 2 * k, last - 2 * k - 1)
                           if k != dev // 2 and (0 < c - kv <= reach or 0 < qd - c <= reach)}
    return out


def neighbours(side, chip):
    x, y = chip % side, chip // side
    return ((y * side + (x + 1) % side, 0), (y * side + (x - 1) % side, 1),
            ((y + 1) % side * side + x, 2), ((y - 1) % side * side + x, 3))


def grow(side, load, src, targets, steep, hop):
    depth = {src: 0}
    edges = []
    missing = set(targets)
    while missing:
        dist = {c: depth[c] * hop for c in depth}
        back = {}
        heap = sorted((d, c) for c, d in dist.items())
        done = set()
        while True:
            d, c = heapq.heappop(heap)
            if c in done:
                continue
            done.add(c)
            if c in missing:
                break
            for nb, way in neighbours(side, c):
                w = d + steep ** load[c, way] + hop
                if nb not in depth and w < dist.get(nb, 1e30):
                    dist[nb], back[nb] = w, (c, way)
                    heapq.heappush(heap, (w, nb))
        path = []
        while c not in depth:
            path.append((back[c][0], back[c][1], c))
            c = back[c][0]
        for p, way, c in reversed(path):
            depth[c] = depth[p] + 1
            edges.append((p, way, c))
            missing.discard(c)
    return edges, depth


def unit_key(side, depth, src, chip, s, h):
    return depth, (src // side - chip // side) % side, (src % side - chip % side) % side, s, h


def arrivals(side, trees, order, hold, lag):
    todo = collections.defaultdict(list)
    for (dev, s, h), (edges, depth) in trees.items():
        onward = collections.defaultdict(list)
        for p, way, c in edges:
            onward[p].append((way, c))
        for c in depth:
            key = unit_key(side, depth[c], dev // 2, c, s, h)
            todo[c, dev % 2].append((order(key), key, (dev, s, h), onward[c]))
    came = {(dev // 2, (dev, s, h)): 0.0 for dev, s, h in trees}
    clock, free, seen = collections.Counter(), collections.Counter(), collections.defaultdict(list)
    queues = {place: sorted(v, key=lambda u: u[:2], reverse=True) for place, v in todo.items()}
    moved = True
    while moved:
        moved = False
        for place, queue in queues.items():
            while queue and (place[0], queue[-1][2]) in came:
                _, key, unit, onward = queue.pop()
                clock[place] = max(clock[place], came[place[0], unit])
                seen[key].append(came[place[0], unit])
                for way, c in onward:
                    free[place, way] = max(clock[place], free[place, way]) + hold
                    came[c, unit] = free[place, way] + lag
                moved = True
    return max(came.values()), {k: sum(v) / len(v) for k, v in seen.items()}


def plan(side, reach, parts, tune):
    steep, hop, seed = tune
    nd = needs(side, reach)
    keys = [(dev, s, h) for h in range(parts) for dev in range(2 * side * side) for s in (0, 1)]
    random.Random(seed).shuffle(keys)
    load, trees, best = collections.Counter(), {}, None
    for _ in range(6):
        for key in keys:
            for p, way, c in trees.get(key, ((), ()))[0]:
                load[p, way] -= 1
            trees[key] = grow(side, load, key[0] // 2, nd[key[0], key[1]], steep, hop)
            for p, way, c in trees[key][0]:
                load[p, way] += 1
        mean = {}
        for _ in range(5):
            end, later = arrivals(side, trees, lambda k: (k[0], round(mean.get(k, 0.0), 3)), 16.9 / parts, 2.5)
            if best is None or end < best[0]:
                best = end, dict(trees), mean
            mean = later
    units = collections.defaultdict(lambda: dict(take=0, send=[0] * 4, keep=0, given=0))
    for (dev, s, h), (edges, depth) in best[1].items():
        src, core = dev // 2, dev % 2

        def unit(c):
            return units[unit_key(side, depth[c], src, c, s, h)]
        for p, way, c in edges:
            unit(c)['take'] |= 1 << (2 * c + core)
            unit(p)['send'][way] |= 1 << (2 * p + core)
        for c in nd[dev, s] | {src}:
            unit(c)['keep'] |= 1 << (2 * c + core)
            unit(c)['given'] |= 1 << (2 * c + 1 - core)
    order = sorted(units.items(), key=lambda kv: (kv[0][0], round(best[2].get(kv[0], 0.0), 3), kv[0]))
    return [(k, v['take'], v['send'], v['keep'], v['given']) for k, v in order]


def multicast_kernel(side, parts, units, x_ref, out_ref, send_sem, recv_sem, chip_send, chip_recv, own_sem):
    me = lax.axis_index('cp')
    core = lax.rem(me, 2)
    chip = me // 2
    cx, cy = lax.rem(chip, side), chip // side
    rows = x_ref.shape[1] // parts
    bit = lax.shift_left(jnp.int32(1), me.astype(jnp.int32))

    def among(mask):
        mask = mask - (1 << 32) if mask >> 31 else mask
        return (bit & jnp.int32(mask)) != 0

    def dev(y, x, c):
        return (lax.rem(cy + y + side, side) * side + lax.rem(cx + x + side, side)) * 2 + c

    partner = dev(0, 0, 1 - core)
    ways = (dev(0, 1, core), dev(0, -1, core), dev(1, 0, core), dev(-1, 0, core))
    barrier = pltpu.get_barrier_semaphore()
    for peer in ways + (partner,):
        pl.semaphore_signal(barrier, inc=1, device_id={'cp': peer}, device_id_type=MESH)
    own = pltpu.make_async_copy(x_ref, out_ref.at[me], own_sem)
    own.start()
    pl.semaphore_wait(barrier, 5)

    sends = []
    slot = {key: k for k, (key, *_) in enumerate(units)}
    for k, ((depth, dy, dx, s, h), take, send, keep, given) in enumerate(units):
        mine = dy == 0 and dx == 0
        block = pl.ds(h * rows, rows)
        here = out_ref.at[dev(dy, dx, core), s, block]
        src = x_ref.at[s, block] if mine else here

        def push():
            for way, mask in enumerate(send):
                if mask:
                    ahead = (dy - (0, 0, 1, -1)[way]) % side, (dx - (1, -1, 0, 0)[way]) % side
                    copy = remote(src, here, send_sem.at[len(sends)], recv_sem.at[slot[depth + 1, *ahead, s, h]], ways[way])
                    sends.append((mask, copy))
                    pl.when(among(mask))(copy.start)
            if keep:
                copy = remote(src, here, chip_send.at[k], chip_recv.at[k], partner)
                sends.append((keep, copy))
                pl.when(among(keep))(copy.start)
        if take:
            pl.when(among(take))(remote(here, here, send_sem.at[0], recv_sem.at[k], partner).wait_recv)
        push()
    for k, ((_, dy, dx, s, h), take, send, keep, given) in enumerate(units):
        there = out_ref.at[dev(dy, dx, 1 - core), s, pl.ds(h * rows, rows)]
        if given:
            pl.when(among(given))(remote(there, there, chip_send.at[k], chip_recv.at[k], partner).wait_recv)
    for mask, copy in sends:
        pl.when(among(mask))(copy.wait_send)
    own.wait()


def multicast(x, n, reach, tune, parts, cid):
    side = math.isqrt(n // 2)
    units = plan(side, reach, parts, tune)
    count = sum(1 for u in units for m in u[2] if m) + len(units)
    sems = [pltpu.SemaphoreType.DMA((c,)) for c in (count, len(units), len(units), len(units))]
    return pl.pallas_call(
        functools.partial(multicast_kernel, side, parts, units),
        out_shape=jax.ShapeDtypeStruct((n,) + x.shape, x.dtype),
        in_specs=[pl.BlockSpec(memory_space=VMEM)],
        out_specs=pl.BlockSpec(memory_space=pltpu.HBM),
        scratch_shapes=sems + [pltpu.SemaphoreType.DMA],
        compiler_params=pltpu.CompilerParams(collective_id=cid, has_side_effects=True),
        name=f'multicast_{reach}',
    )(x)


def dot_nt(a, b):
    return lax.dot_general(a, b, (((1,), (1,)), ((), ())), preferred_element_type=F32)


def dot_nn(a, b):
    return lax.dot_general(a, b, (((1,), (0,)), ((), ())), preferred_element_type=F32)


def query_kernel(pieces, plen, hd, scale, meta, a_ref, docs_ref, mine_ref, g_ref, o_ref, dq_ref, ld_ref,
                 kv, p_s, q2, do2, m_s, l_s, acc, sem):
    wide = 2 * plen
    for t in range(2):
        c, lo = meta[t], meta[2 + t]
        blocks = (c - lo + 2) // 2

        def fetch(i):
            p = jnp.minimum(lo + i, c)
            far = (p >= pieces // 2).astype(jnp.int32)
            d = jnp.where(far == 1, pieces - 1 - p, p)
            return pltpu.make_async_copy(g_ref.at[d, far, :, pl.ds(0, 2 * hd)], kv.at[pl.ds(i * plen, plen)], sem.at[i])

        def issue(i, _):
            fetch(i).start()
            return 0
        lax.fori_loop(0, 2 * blocks, issue, 0)
        for h in range(2):
            rows = pl.ds(h * plen, plen)
            q2[rows, :] = a_ref[1 - t, :, pl.ds((2 + h) * hd, hd)]
            do2[rows, :] = a_ref[1 - t, :, pl.ds((4 + h) * hd, hd)]
        m_s[...] = jnp.full_like(m_s, NEG_BIG)
        l_s[...] = jnp.zeros_like(l_s)
        acc[...] = jnp.zeros_like(acc)
        doc = mine_ref[t]
        doc = jnp.concatenate([doc, doc], axis=0)
        row = lax.broadcasted_iota(jnp.int32, (plen, 1), 0) + c * plen
        row = jnp.concatenate([row, row], axis=0)

        def keys(i):
            return pl.ds(pl.multiple_of(i * wide, wide), wide)

        def scores(i):
            s = dot_nt(q2[...], kv[keys(i), pl.ds(0, hd)]) * scale
            p = lo + 2 * i
            key_doc = jnp.concatenate([docs_ref[pl.ds(p, 1), :], docs_ref[pl.ds(jnp.minimum(p + 1, c), 1), :]], axis=1)
            col = lax.broadcasted_iota(jnp.int32, (1, wide), 1) + p * plen
            return jnp.where((key_doc == doc) & (col <= row), s, NEG_BIG)

        def sweep_norm(i, _):
            fetch(2 * i).wait()
            fetch(2 * i + 1).wait()
            s = scores(i)
            parts = [s[:, k:k + 128] for k in range(0, wide, 128)]
            m = m_s[...]
            m_new = jnp.maximum(m, functools.reduce(jnp.maximum, parts))
            l_s[...] = l_s[...] * jnp.exp(m - m_new) + sum(jnp.exp(part - m_new) for part in parts)
            m_s[...] = m_new
            return 0
        lax.fori_loop(0, blocks, sweep_norm, 0)
        top = jnp.max(m_s[...], axis=1, keepdims=True)
        total = jnp.sum(l_s[...] * jnp.exp(m_s[...] - top), axis=1, keepdims=True)
        log_norm = top + jnp.log(total)

        def sweep_out(i, _):
            p = jnp.exp(scores(i) - log_norm).astype(BF16)
            p_s[i] = p
            acc[...] += dot_nn(p, kv[keys(i), pl.ds(hd, hd)])
            return 0
        lax.fori_loop(0, blocks, sweep_out, 0)
        out = acc[...].astype(BF16)
        delta = jnp.sum(do2[...].astype(F32) * out.astype(F32), axis=1, keepdims=True)
        acc[...] = jnp.zeros_like(acc)

        def sweep_dq(i, _):
            dp = dot_nt(do2[...], kv[keys(i), pl.ds(hd, hd)])
            ds = (p_s[i].astype(F32) * (dp - delta)).astype(BF16)
            acc[...] += dot_nn(ds, kv[keys(i), pl.ds(0, hd)])
            return 0
        lax.fori_loop(0, blocks, sweep_dq, 0)
        dq = (acc[...] * scale).astype(BF16)
        for h in range(2):
            o_ref[pl.ds(t * plen, plen), pl.ds(h * hd, hd)] = out[h * plen:(h + 1) * plen]
            dq_ref[pl.ds(t * plen, plen), pl.ds(h * hd, hd)] = dq[h * plen:(h + 1) * plen]
        ld_ref[pl.ds(2 * t, 1), :] = jnp.transpose(jnp.broadcast_to(log_norm, (wide, 128)))[0:1]
        ld_ref[pl.ds(2 * t + 1, 1), :] = jnp.transpose(jnp.broadcast_to(delta, (wide, 128)))[0:1]


def key_kernel(pieces, plen, hd, scale, meta, a_ref, docs_ref, mine_ref, ld_ref, g_ref, dk_ref, dv_ref,
               qd, kt, vt, dk_acc, dv_acc, sem):
    for t in range(2):
        c, hi = meta[t], meta[4 + t]
        count = hi - c + 1

        def place(i):
            p = c + i
            far = (p >= pieces // 2).astype(jnp.int32)
            return p, far, jnp.where(far == 1, pieces - 1 - p, p)

        def fetch(i):
            _, far, d = place(i)
            b = lax.rem(i, 3)
            return [pltpu.make_async_copy(g_ref.at[d, 1 - far, :, pl.ds((2 + k) * hd, hd)],
                                          qd.at[b, k // 2, pl.ds((k % 2) * plen, plen)], sem.at[b, k]) for k in range(4)]

        def start(i):
            for copy in fetch(i):
                copy.start()

        start(0)
        pl.when(count > 1)(lambda: start(1))
        kt[...] = a_ref[t, :, pl.ds(0, hd)]
        vt[...] = a_ref[t, :, pl.ds(hd, hd)]
        dk_acc[...] = jnp.zeros_like(dk_acc)
        dv_acc[...] = jnp.zeros_like(dv_acc)
        doc = mine_ref[t]
        key = lax.broadcasted_iota(jnp.int32, (plen, 1), 0)

        def sweep(i, _):
            pl.when(i + 2 < count)(lambda: start(i + 2))
            for copy in fetch(i):
                copy.wait()
            b = lax.rem(i, 3)
            p_idx, far, d = place(i)
            col = lax.broadcasted_iota(jnp.int32, (1, plen), 1) + i * plen
            seen = (docs_ref[pl.ds(p_idx, 1), :] == doc) & (col >= key)
            seen = jnp.concatenate([seen, seen], axis=1)
            st = jnp.where(seen, dot_nt(kt[...], qd[b, 0]) * scale, NEG_BIG)
            dpt = dot_nt(vt[...], qd[b, 1])
            pt = jnp.exp(st - ld_ref[d, pl.ds(2 * far, 1), :]).astype(BF16)
            dst = (pt.astype(F32) * (dpt - ld_ref[d, pl.ds(2 * far + 1, 1), :])).astype(BF16)
            dv_acc[...] += dot_nn(pt, qd[b, 1])
            dk_acc[...] += dot_nn(dst, qd[b, 0])
            return 0
        lax.fori_loop(0, count, sweep, 0)
        dk_ref[pl.ds(t * plen, plen), :] = (dk_acc[...] * scale).astype(BF16)
        dv_ref[pl.ds(t * plen, plen), :] = dv_acc[...].astype(BF16)


def solution(mesh):
    n = mesh.shape['cp']
    row_spec = P(('dp', 'cp'))
    full_spec = P()

    def local_layer(x_in, dy_in, doc_id, w_q, w_k, w_v, w_o):
        tok, d_model = x_in.shape
        heads, hd = w_q.shape[1], w_q.shape[2]
        plen = tok // 2
        pieces = 2 * n
        seq = tok * n
        scale = hd ** -0.5
        me = lax.axis_index('cp')
        wq = w_q.reshape(d_model, heads * hd)
        wk = w_k.reshape(d_model, hd)
        wv = w_v.reshape(d_model, hd)
        wo = w_o.reshape(heads * hd, d_model)

        lane = 128
        doc_pad = jnp.pad(doc_id.reshape(tok // lane, lane), ((0, 8 - tok // lane), (0, 0)))
        a_loc, docs = project(doc_pad, x_in, dy_in, wk, wv, wq, wo, n, 1)
        docs = docs[:, :tok // lane].reshape(n, 2, plen)
        docs = jnp.concatenate([docs[:, 0], docs[::-1, 1]])
        first, last = docs[:, 0], docs[:, plen - 1]
        begun = jnp.sum((last[None, :] < first[:, None]).astype(jnp.int32), axis=1)
        ended = jnp.sum((first[None, :] <= last[:, None]).astype(jnp.int32), axis=1) - 1
        own = jnp.stack([me, pieces - 1 - me]).astype(jnp.int32)
        meta = jnp.concatenate([own, begun[own], ended[own]])
        mine = doc_id.reshape(2, plen, 1)

        span = jnp.max(jnp.arange(pieces) - begun)
        level = sum((span <= r).astype(jnp.int32) for r in REACHES)
        g_all = lax.switch(level, [functools.partial(multicast, n=n, reach=r, tune=TUNES[i], parts=PARTS, cid=4 + i)
                                   for i, r in enumerate((pieces,) + REACHES)], a_loc)

        smem = pl.BlockSpec(memory_space=pltpu.SMEM)
        vmem = pl.BlockSpec(memory_space=VMEM)
        hbm = pl.BlockSpec(memory_space=pltpu.HBM)
        o_loc, dq_loc, ld = pl.pallas_call(
            functools.partial(query_kernel, pieces, plen, hd, scale),
            out_shape=(jax.ShapeDtypeStruct((tok, heads * hd), BF16), jax.ShapeDtypeStruct((tok, heads * hd), BF16),
                       jax.ShapeDtypeStruct((4, 2 * plen), F32)),
            in_specs=[smem, vmem, vmem, vmem, hbm], out_specs=(vmem, vmem, vmem),
            scratch_shapes=[VMEM((pieces * plen, 2 * hd), BF16), VMEM((n, 2 * plen, 2 * plen), BF16),
                            VMEM((2 * plen, hd), BF16), VMEM((2 * plen, hd), BF16), VMEM((2 * plen, 128), F32),
                            VMEM((2 * plen, 128), F32), VMEM((2 * plen, hd), F32), pltpu.SemaphoreType.DMA((pieces,))],
            compiler_params=pltpu.CompilerParams(vmem_limit_bytes=60 * 1024 * 1024),
            name='query_side',
        )(meta, a_loc, docs, mine, g_all)
        ld_all, y_out = exchange(ld, o_loc, wo, n, hd, 3)
        dk_loc, dv_loc = pl.pallas_call(
            functools.partial(key_kernel, pieces, plen, hd, scale),
            out_shape=(jax.ShapeDtypeStruct((tok, hd), BF16), jax.ShapeDtypeStruct((tok, hd), BF16)),
            in_specs=[smem, vmem, vmem, vmem, vmem, hbm], out_specs=(vmem, vmem),
            scratch_shapes=[VMEM((3, 2, 2 * plen, hd), BF16), VMEM((plen, hd), BF16), VMEM((plen, hd), BF16),
                            VMEM((plen, hd), F32), VMEM((plen, hd), F32), pltpu.SemaphoreType.DMA((3, 4))],
            name='key_side',
        )(meta, a_loc, docs, mine, ld_all, g_all)
        nt = (((1,), (1,)), ((), ()))
        dx = (lax.dot_general(dq_loc, wq, nt, preferred_element_type=F32)
              + lax.dot_general(dk_loc, wk, nt, preferred_element_type=F32)
              + lax.dot_general(dv_loc, wv, nt, preferred_element_type=F32))
        return y_out, dx.astype(BF16)

    return jax.shard_map(local_layer, mesh=mesh,
                         in_specs=(row_spec, row_spec, row_spec, full_spec, full_spec, full_spec, full_spec),
                         out_specs=(row_spec, row_spec), check_vma=False)
```

```python
import collections
import functools
import heapq
import math
import random

import jax
import jax.numpy as jnp
from jax import lax
from jax.experimental import pallas as pl
from jax.experimental.pallas import tpu as pltpu
from jax.sharding import PartitionSpec as P

NEG_BIG = -1.0e30
MESH = pl.DeviceIdType.MESH
VMEM = pltpu.VMEM
F32 = jnp.float32
REACHES = (20, 16, 11)
TUNES = ((1.05, 0.3, 52), (1.05, 1.0, 15), (1.2, 3.0, 49), (1.2, 3.0, 29))
PARTS = 2
BF16 = jnp.bfloat16


def remote(src, dst, send_sem, recv_sem, dev):
    return pltpu.make_async_remote_copy(src_ref=src, dst_ref=dst, send_sem=send_sem, recv_sem=recv_sem,
                                        device_id={'cp': dev}, device_id_type=MESH)


def exchange_kernel(n, hd, ld_ref, o_ref, wo_ref, all_ref, y_ref, wo_v, y_v, load_sem, store_sem, send_sem, recv_sem, own_sem):
    me = lax.axis_index('cp')
    barrier = pltpu.get_barrier_semaphore()
    load = pltpu.make_async_copy(wo_ref, wo_v, load_sem)
    load.start()

    def greet(off, _):
        pl.semaphore_signal(barrier, inc=1, device_id={'cp': lax.rem(me + off, n)}, device_id_type=MESH)
        return 0
    lax.fori_loop(1, n, greet, 0)
    own = pltpu.make_async_copy(ld_ref, all_ref.at[me], own_sem)
    own.start()
    pl.semaphore_wait(barrier, n - 1)

    def send(off, _):
        remote(ld_ref, all_ref.at[me], send_sem.at[off], recv_sem.at[off], lax.rem(me + off, n)).start()
        return 0
    lax.fori_loop(1, n, send, 0)
    load.wait()
    cols = 2 * hd
    count = y_ref.shape[1] // cols

    def store(j):
        at = pl.ds(pl.multiple_of(j * cols, cols), cols)
        return pltpu.make_async_copy(y_v.at[:, at], y_ref.at[:, at], store_sem.at[j])

    def column(j, _):
        at = pl.ds(pl.multiple_of(j * cols, cols), cols)
        y_v[:, at] = dot_nn(o_ref[...], wo_v[:, at]).astype(BF16)
        store(j).start()
        return 0
    lax.fori_loop(0, count, column, 0)
    own.wait()

    def settle(off, _):
        src = lax.rem(me + n - off, n)
        copy = remote(ld_ref, all_ref.at[src], send_sem.at[off], recv_sem.at[off], lax.rem(me + off, n))
        copy.wait_send()
        copy.wait_recv()
        return 0
    lax.fori_loop(1, n, settle, 0)

    def stored(j, _):
        store(j).wait()
        return 0
    lax.fori_loop(0, count, stored, 0)


def exchange(ld, o, wo, n, hd, cid):
    tok, d_model = o.shape[0], wo.shape[1]
    vmem, hbm = pl.BlockSpec(memory_space=VMEM), pl.BlockSpec(memory_space=pltpu.HBM)
    dma = pltpu.SemaphoreType.DMA
    return pl.pallas_call(
        functools.partial(exchange_kernel, n, hd),
        out_shape=(jax.ShapeDtypeStruct((n,) + ld.shape, ld.dtype), jax.ShapeDtypeStruct((tok, d_model), BF16)),
        in_specs=[vmem, vmem, hbm], out_specs=(vmem, hbm),
        scratch_shapes=[VMEM(wo.shape, BF16), VMEM((tok, d_model), BF16), dma, dma((d_model // (2 * hd),)), dma((n,)), dma((n,)), dma],
        compiler_params=pltpu.CompilerParams(collective_id=cid, has_side_effects=True, vmem_limit_bytes=16 * 1024 * 1024),
        name='exchange',
    )(ld, o, wo)


def project_kernel(n, hd, doc_ref, x_ref, dy_ref, wk_ref, wv_ref, wq_ref, wo_ref, out_ref, docs_ref,
                   x_v, dy_v, kv_v, wq_v, wo_v, load_sem, send_sem, recv_sem, own_sem):
    me = lax.axis_index('cp')
    barrier = pltpu.get_barrier_semaphore()

    def greet(off, _):
        pl.semaphore_signal(barrier, inc=1, device_id={'cp': lax.rem(me + off, n)}, device_id_type=MESH)
        return 0
    lax.fori_loop(1, n, greet, 0)
    loads = [pltpu.make_async_copy(src, dst, load_sem.at[i]) for i, (src, dst) in enumerate(
        ((x_ref, x_v), (wk_ref, kv_v.at[0]), (wv_ref, kv_v.at[1]), (wq_ref, wq_v), (dy_ref, dy_v), (wo_ref, wo_v)))]
    for load in loads:
        load.start()
    own = pltpu.make_async_copy(doc_ref, docs_ref.at[me], own_sem)
    own.start()
    half = x_ref.shape[0] // 2

    def fill(kind, src, weights, dot, col):
        def rows(t, _):
            out_ref[jnp.abs(t - kind), :, pl.ds(col, hd)] = dot(src[pl.ds(t * half, half), :], weights).astype(BF16)
            return 0
        lax.fori_loop(0, 2, rows, 0)

    loads[0].wait()
    for i in range(2):
        loads[1 + i].wait()
        fill(0, x_v, kv_v[i], dot_nn, i * hd)
    pl.semaphore_wait(barrier, n - 1)

    def send(off, _):
        remote(doc_ref, docs_ref.at[me], send_sem.at[off], recv_sem.at[off], lax.rem(me + off, n)).start()
        return 0
    lax.fori_loop(1, n, send, 0)
    loads[3].wait()
    for h in range(2):
        fill(1, x_v, wq_v[:, pl.ds(h * hd, hd)], dot_nn, (2 + h) * hd)
    loads[4].wait()
    loads[5].wait()
    for h in range(2):
        fill(1, dy_v, wo_v[pl.ds(h * hd, hd), :], dot_nt, (4 + h) * hd)
    own.wait()

    def settle(off, _):
        src = lax.rem(me + n - off, n)
        copy = remote(doc_ref, docs_ref.at[src], send_sem.at[off], recv_sem.at[off], lax.rem(me + off, n))
        copy.wait_send()
        copy.wait_recv()
        return 0
    lax.fori_loop(1, n, settle, 0)


def project(doc, x, dy, wk, wv, wq, wo, n, cid):
    tok, d_model = x.shape
    hd = wk.shape[1]
    vmem, hbm = pl.BlockSpec(memory_space=VMEM), pl.BlockSpec(memory_space=pltpu.HBM)
    return pl.pallas_call(
        functools.partial(project_kernel, n, hd),
        out_shape=(jax.ShapeDtypeStruct((2, tok // 2, 6 * hd), BF16), jax.ShapeDtypeStruct((n,) + doc.shape, doc.dtype)),
        in_specs=[vmem] + [hbm] * 6, out_specs=(vmem, vmem),
        scratch_shapes=[VMEM((tok, d_model), BF16), VMEM((tok, d_model), BF16), VMEM((2, d_model, hd), BF16),
                        VMEM((d_model, 2 * hd), BF16), VMEM((2 * hd, d_model), BF16), pltpu.SemaphoreType.DMA((6,)),
                        pltpu.SemaphoreType.DMA((n,)), pltpu.SemaphoreType.DMA((n,)), pltpu.SemaphoreType.DMA],
        compiler_params=pltpu.CompilerParams(collective_id=cid, has_side_effects=True, vmem_limit_bytes=48 * 1024 * 1024),
        name='project',
    )(doc, x, dy, wk, wv, wq, wo)


def small_gather(x, n, cid):
    return pl.pallas_call(
        functools.partial(small_gather_kernel, n),
        out_shape=jax.ShapeDtypeStruct((n,) + x.shape, x.dtype),
        in_specs=[pl.BlockSpec(memory_space=VMEM)],
        out_specs=pl.BlockSpec(memory_space=VMEM),
        scratch_shapes=[pltpu.SemaphoreType.DMA((n,)), pltpu.SemaphoreType.DMA((n,)), pltpu.SemaphoreType.DMA],
        compiler_params=pltpu.CompilerParams(collective_id=cid, has_side_effects=True),
        name=f'small_gather_{cid}',
    )(x)


def needs(side, reach):
    chips = side * side
    last = 4 * chips - 1
    out = {}
    for dev in range(2 * chips):
        for s in (0, 1):
            kv, qd = (dev, last - dev) if s == 0 else (last - dev, dev)
            out[dev, s] = {k for k in range(chips) for c in (2 * k, 2 * k + 1, last - 2 * k, last - 2 * k - 1)
                           if k != dev // 2 and (0 < c - kv <= reach or 0 < qd - c <= reach)}
    return out


def neighbours(side, chip):
    x, y = chip % side, chip // side
    return ((y * side + (x + 1) % side, 0), (y * side + (x - 1) % side, 1),
            ((y + 1) % side * side + x, 2), ((y - 1) % side * side + x, 3))


def grow(side, load, src, targets, steep, hop):
    depth = {src: 0}
    edges = []
    missing = set(targets)
    while missing:
        dist = {c: depth[c] * hop for c in depth}
        back = {}
        heap = sorted((d, c) for c, d in dist.items())
        done = set()
        while True:
            d, c = heapq.heappop(heap)
            if c in done:
                continue
            done.add(c)
            if c in missing:
                break
            for nb, way in neighbours(side, c):
                w = d + steep ** load[c, way] + hop
                if nb not in depth and w < dist.get(nb, 1e30):
                    dist[nb], back[nb] = w, (c, way)
                    heapq.heappush(heap, (w, nb))
        path = []
        while c not in depth:
            path.append((back[c][0], back[c][1], c))
            c = back[c][0]
        for p, way, c in reversed(path):
            depth[c] = depth[p] + 1
            edges.append((p, way, c))
            missing.discard(c)
    return edges, depth


def unit_key(side, depth, src, chip, s, h):
    return depth, (src // side - chip // side) % side, (src % side - chip % side) % side, s, h


def arrivals(side, trees, order, hold, lag):
    todo = collections.defaultdict(list)
    for (dev, s, h), (edges, depth) in trees.items():
        onward = collections.defaultdict(list)
        for p, way, c in edges:
            onward[p].append((way, c))
        for c in depth:
            key = unit_key(side, depth[c], dev // 2, c, s, h)
            todo[c, dev % 2].append((order(key), key, (dev, s, h), onward[c]))
    came = {(dev // 2, (dev, s, h)): 0.0 for dev, s, h in trees}
    clock, free, seen = collections.Counter(), collections.Counter(), collections.defaultdict(list)
    queues = {place: sorted(v, key=lambda u: u[:2], reverse=True) for place, v in todo.items()}
    moved = True
    while moved:
        moved = False
        for place, queue in queues.items():
            while queue and (place[0], queue[-1][2]) in came:
                _, key, unit, onward = queue.pop()
                clock[place] = max(clock[place], came[place[0], unit])
                seen[key].append(came[place[0], unit])
                for way, c in onward:
                    free[place, way] = max(clock[place], free[place, way]) + hold
                    came[c, unit] = free[place, way] + lag
                moved = True
    return max(came.values()), {k: sum(v) / len(v) for k, v in seen.items()}


def plan(side, reach, parts, tune):
    steep, hop, seed = tune
    nd = needs(side, reach)
    keys = [(dev, s, h) for h in range(parts) for dev in range(2 * side * side) for s in (0, 1)]
    random.Random(seed).shuffle(keys)
    load, trees, best = collections.Counter(), {}, None
    for _ in range(6):
        for key in keys:
            for p, way, c in trees.get(key, ((), ()))[0]:
                load[p, way] -= 1
            trees[key] = grow(side, load, key[0] // 2, nd[key[0], key[1]], steep, hop)
            for p, way, c in trees[key][0]:
                load[p, way] += 1
        mean = {}
        for _ in range(5):
            end, later = arrivals(side, trees, lambda k: (k[0], round(mean.get(k, 0.0), 3)), 16.9 / parts, 2.5)
            if best is None or end < best[0]:
                best = end, dict(trees), mean
            mean = later
    units = collections.defaultdict(lambda: dict(take=0, send=[0] * 4, keep=0, given=0))
    for (dev, s, h), (edges, depth) in best[1].items():
        src, core = dev // 2, dev % 2

        def unit(c):
            return units[unit_key(side, depth[c], src, c, s, h)]
        for p, way, c in edges:
            unit(c)['take'] |= 1 << (2 * c + core)
            unit(p)['send'][way] |= 1 << (2 * p + core)
        for c in nd[dev, s] | {src}:
            unit(c)['keep'] |= 1 << (2 * c + core)
            unit(c)['given'] |= 1 << (2 * c + 1 - core)
    order = sorted(units.items(), key=lambda kv: (kv[0][0], round(best[2].get(kv[0], 0.0), 3), kv[0]))
    return [(k, v['take'], v['send'], v['keep'], v['given']) for k, v in order]


def multicast_kernel(side, parts, units, x_ref, out_ref, send_sem, recv_sem, chip_send, chip_recv, own_sem):
    me = lax.axis_index('cp')
    core = lax.rem(me, 2)
    chip = me // 2
    cx, cy = lax.rem(chip, side), chip // side
    rows = x_ref.shape[1] // parts
    bit = lax.shift_left(jnp.int32(1), me.astype(jnp.int32))

    def among(mask):
        mask = mask - (1 << 32) if mask >> 31 else mask
        return (bit & jnp.int32(mask)) != 0

    def dev(y, x, c):
        return (lax.rem(cy + y + side, side) * side + lax.rem(cx + x + side, side)) * 2 + c

    partner = dev(0, 0, 1 - core)
    ways = (dev(0, 1, core), dev(0, -1, core), dev(1, 0, core), dev(-1, 0, core))
    barrier = pltpu.get_barrier_semaphore()
    for peer in ways + (partner,):
        pl.semaphore_signal(barrier, inc=1, device_id={'cp': peer}, device_id_type=MESH)
    own = pltpu.make_async_copy(x_ref, out_ref.at[me], own_sem)
    own.start()
    pl.semaphore_wait(barrier, 5)

    sends = []
    slot = {key: k for k, (key, *_) in enumerate(units)}
    for k, ((depth, dy, dx, s, h), take, send, keep, given) in enumerate(units):
        mine = dy == 0 and dx == 0
        block = pl.ds(h * rows, rows)
        here = out_ref.at[dev(dy, dx, core), s, block]
        src = x_ref.at[s, block] if mine else here

        def push():
            for way, mask in enumerate(send):
                if mask:
                    ahead = (dy - (0, 0, 1, -1)[way]) % side, (dx - (1, -1, 0, 0)[way]) % side
                    copy = remote(src, here, send_sem.at[len(sends)], recv_sem.at[slot[depth + 1, *ahead, s, h]], ways[way])
                    sends.append((mask, copy))
                    pl.when(among(mask))(copy.start)
            if keep:
                copy = remote(src, here, chip_send.at[k], chip_recv.at[k], partner)
                sends.append((keep, copy))
                pl.when(among(keep))(copy.start)
        if take:
            pl.when(among(take))(remote(here, here, send_sem.at[0], recv_sem.at[k], partner).wait_recv)
        push()
    for k, ((_, dy, dx, s, h), take, send, keep, given) in enumerate(units):
        there = out_ref.at[dev(dy, dx, 1 - core), s, pl.ds(h * rows, rows)]
        if given:
            pl.when(among(given))(remote(there, there, chip_send.at[k], chip_recv.at[k], partner).wait_recv)
    for mask, copy in sends:
        pl.when(among(mask))(copy.wait_send)
    own.wait()


def multicast(x, n, reach, tune, parts, cid):
    side = math.isqrt(n // 2)
    units = plan(side, reach, parts, tune)
    count = sum(1 for u in units for m in u[2] if m) + len(units)
    sems = [pltpu.SemaphoreType.DMA((c,)) for c in (count, len(units), len(units), len(units))]
    return pl.pallas_call(
        functools.partial(multicast_kernel, side, parts, units),
        out_shape=jax.ShapeDtypeStruct((n,) + x.shape, x.dtype),
        in_specs=[pl.BlockSpec(memory_space=VMEM)],
        out_specs=pl.BlockSpec(memory_space=pltpu.HBM),
        scratch_shapes=sems + [pltpu.SemaphoreType.DMA],
        compiler_params=pltpu.CompilerParams(collective_id=cid, has_side_effects=True, vmem_limit_bytes=8 * 1024 * 1024),
        name=f'multicast_{reach}',
    )(x)


def dot_nt(a, b):
    return lax.dot_general(a, b, (((1,), (1,)), ((), ())), preferred_element_type=F32)


def dot_nn(a, b):
    return lax.dot_general(a, b, (((1,), (0,)), ((), ())), preferred_element_type=F32)


def column(row):
    return jnp.transpose(jnp.broadcast_to(row.astype(F32), (128, row.shape[1])))[:, 0:1].astype(jnp.int32)


def query_kernel(pieces, plen, hd, scale, meta, a_ref, docs_ref, g_ref, o_ref, dq_ref, ld_ref,
                 kv, p_s, q2, do2, m_s, l_s, acc, sem):
    wide = 2 * plen
    for t in range(2):
        c, lo = meta[t], meta[2 + t]
        blocks = (c - lo + 2) // 2

        def fetch(i):
            p = jnp.minimum(lo + i, c)
            far = (p >= pieces // 2).astype(jnp.int32)
            d = jnp.where(far == 1, pieces - 1 - p, p)
            return pltpu.make_async_copy(g_ref.at[d, far, :, pl.ds(0, 2 * hd)], kv.at[pl.ds(i * plen, plen)], sem.at[i])

        def issue(i, _):
            fetch(i).start()
            return 0
        lax.fori_loop(0, 2 * blocks, issue, 0)
        for h in range(2):
            rows = pl.ds(h * plen, plen)
            q2[rows, :] = a_ref[1 - t, :, pl.ds((2 + h) * hd, hd)]
            do2[rows, :] = a_ref[1 - t, :, pl.ds((4 + h) * hd, hd)]
        m_s[...] = jnp.full_like(m_s, NEG_BIG)
        l_s[...] = jnp.zeros_like(l_s)
        acc[...] = jnp.zeros_like(acc)
        doc = column(docs_ref[pl.ds(c, 1), :])
        doc = jnp.concatenate([doc, doc], axis=0)
        row = lax.broadcasted_iota(jnp.int32, (plen, 1), 0) + c * plen
        row = jnp.concatenate([row, row], axis=0)

        def keys(i):
            return pl.ds(pl.multiple_of(i * wide, wide), wide)

        def scores(i):
            s = dot_nt(q2[...], kv[keys(i), pl.ds(0, hd)]) * scale
            p = lo + 2 * i
            key_doc = jnp.concatenate([docs_ref[pl.ds(p, 1), :], docs_ref[pl.ds(jnp.minimum(p + 1, c), 1), :]], axis=1)
            col = lax.broadcasted_iota(jnp.int32, (1, wide), 1) + p * plen
            return jnp.where((key_doc == doc) & (col <= row), s, NEG_BIG)

        def sweep_norm(i, _):
            fetch(2 * i).wait()
            fetch(2 * i + 1).wait()
            s = scores(i)
            parts = [s[:, k:k + 128] for k in range(0, wide, 128)]
            m = m_s[...]
            m_new = jnp.maximum(m, functools.reduce(jnp.maximum, parts))
            l_s[...] = l_s[...] * jnp.exp(m - m_new) + sum(jnp.exp(part - m_new) for part in parts)
            m_s[...] = m_new
            return 0
        lax.fori_loop(0, blocks, sweep_norm, 0)
        top = jnp.max(m_s[...], axis=1, keepdims=True)
        total = jnp.sum(l_s[...] * jnp.exp(m_s[...] - top), axis=1, keepdims=True)
        log_norm = top + jnp.log(total)

        def sweep_out(i, _):
            p = jnp.exp(scores(i) - log_norm).astype(BF16)
            p_s[i] = p
            acc[...] += dot_nn(p, kv[keys(i), pl.ds(hd, hd)])
            return 0
        lax.fori_loop(0, blocks, sweep_out, 0)
        out = acc[...].astype(BF16)
        delta = jnp.sum(do2[...].astype(F32) * out.astype(F32), axis=1, keepdims=True)
        acc[...] = jnp.zeros_like(acc)

        def sweep_dq(i, _):
            dp = dot_nt(do2[...], kv[keys(i), pl.ds(hd, hd)])
            ds = (p_s[i].astype(F32) * (dp - delta)).astype(BF16)
            acc[...] += dot_nn(ds, kv[keys(i), pl.ds(0, hd)])
            return 0
        lax.fori_loop(0, blocks, sweep_dq, 0)
        dq = (acc[...] * scale).astype(BF16)
        for h in range(2):
            o_ref[pl.ds(t * plen, plen), pl.ds(h * hd, hd)] = out[h * plen:(h + 1) * plen]
            dq_ref[pl.ds(t * plen, plen), pl.ds(h * hd, hd)] = dq[h * plen:(h + 1) * plen]
        ld_ref[pl.ds(2 * t, 1), :] = jnp.transpose(jnp.broadcast_to(log_norm, (wide, 128)))[0:1]
        ld_ref[pl.ds(2 * t + 1, 1), :] = jnp.transpose(jnp.broadcast_to(delta, (wide, 128)))[0:1]


def key_kernel(pieces, plen, hd, scale, meta, a_ref, docs_ref, ld_ref, g_ref, dk_ref, dv_ref,
               qd, kt, vt, dk_acc, dv_acc, sem):
    for t in range(2):
        c, hi = meta[t], meta[4 + t]
        count = hi - c + 1

        def place(i):
            p = c + i
            far = (p >= pieces // 2).astype(jnp.int32)
            return p, far, jnp.where(far == 1, pieces - 1 - p, p)

        def fetch(i):
            _, far, d = place(i)
            b = lax.rem(i, 3)
            return [pltpu.make_async_copy(g_ref.at[d, 1 - far, :, pl.ds((2 + k) * hd, hd)],
                                          qd.at[b, k // 2, pl.ds((k % 2) * plen, plen)], sem.at[b, k]) for k in range(4)]

        def start(i):
            for copy in fetch(i):
                copy.start()

        start(0)
        pl.when(count > 1)(lambda: start(1))
        kt[...] = a_ref[t, :, pl.ds(0, hd)]
        vt[...] = a_ref[t, :, pl.ds(hd, hd)]
        dk_acc[...] = jnp.zeros_like(dk_acc)
        dv_acc[...] = jnp.zeros_like(dv_acc)
        doc = column(docs_ref[pl.ds(c, 1), :])
        key = lax.broadcasted_iota(jnp.int32, (plen, 1), 0)

        def sweep(i, _):
            pl.when(i + 2 < count)(lambda: start(i + 2))
            for copy in fetch(i):
                copy.wait()
            b = lax.rem(i, 3)
            p_idx, far, d = place(i)
            col = lax.broadcasted_iota(jnp.int32, (1, plen), 1) + i * plen
            seen = (docs_ref[pl.ds(p_idx, 1), :] == doc) & (col >= key)
            seen = jnp.concatenate([seen, seen], axis=1)
            st = jnp.where(seen, dot_nt(kt[...], qd[b, 0]) * scale, NEG_BIG)
            dpt = dot_nt(vt[...], qd[b, 1])
            pt = jnp.exp(st - ld_ref[d, pl.ds(2 * far, 1), :]).astype(BF16)
            dst = (pt.astype(F32) * (dpt - ld_ref[d, pl.ds(2 * far + 1, 1), :])).astype(BF16)
            dv_acc[...] += dot_nn(pt, qd[b, 1])
            dk_acc[...] += dot_nn(dst, qd[b, 0])
            return 0
        lax.fori_loop(0, count, sweep, 0)
        dk_ref[pl.ds(t * plen, plen), :] = (dk_acc[...] * scale).astype(BF16)
        dv_ref[pl.ds(t * plen, plen), :] = dv_acc[...].astype(BF16)


def solution(mesh):
    n = mesh.shape['cp']
    row_spec = P(('dp', 'cp'))
    full_spec = P()

    def local_layer(x_in, dy_in, doc_id, w_q, w_k, w_v, w_o):
        tok, d_model = x_in.shape
        heads, hd = w_q.shape[1], w_q.shape[2]
        plen = tok // 2
        pieces = 2 * n
        seq = tok * n
        scale = hd ** -0.5
        me = lax.axis_index('cp')
        wq = w_q.reshape(d_model, heads * hd)
        wk = w_k.reshape(d_model, hd)
        wv = w_v.reshape(d_model, hd)
        wo = w_o.reshape(heads * hd, d_model)

        lane = 128
        doc_pad = jnp.pad(doc_id.reshape(tok // lane, lane), ((0, 8 - tok // lane), (0, 0)))
        a_loc, docs = project(doc_pad, x_in, dy_in, wk, wv, wq, wo, n, 1)
        docs = docs[:, :tok // lane].reshape(n, 2, plen)
        docs = jnp.concatenate([docs[:, 0], docs[::-1, 1]])
        first, last = docs[:, 0], docs[:, plen - 1]
        begun = jnp.sum((last[None, :] < first[:, None]).astype(jnp.int32), axis=1)
        opens, closes = (f(doc_id.reshape(2, plen), axis=1) for f in (jnp.min, jnp.max))
        meta = jnp.concatenate([
            jnp.stack([me, pieces - 1 - me]).astype(jnp.int32),
            jnp.sum((last[None, :] < opens[:, None]).astype(jnp.int32), axis=1),
            jnp.sum((first[None, :] <= closes[:, None]).astype(jnp.int32), axis=1) - 1])
        span = jnp.max(jnp.arange(pieces) - begun)
        level = sum((span <= r).astype(jnp.int32) for r in REACHES)
        g_all = lax.switch(level, [functools.partial(multicast, n=n, reach=r, tune=TUNES[i], parts=PARTS, cid=4 + i)
                                   for i, r in enumerate((pieces,) + REACHES)], a_loc)

        smem = pl.BlockSpec(memory_space=pltpu.SMEM)
        vmem = pl.BlockSpec(memory_space=VMEM)
        hbm = pl.BlockSpec(memory_space=pltpu.HBM)
        o_loc, dq_loc, ld = pl.pallas_call(
            functools.partial(query_kernel, pieces, plen, hd, scale),
            out_shape=(jax.ShapeDtypeStruct((tok, heads * hd), BF16), jax.ShapeDtypeStruct((tok, heads * hd), BF16),
                       jax.ShapeDtypeStruct((4, 2 * plen), F32)),
            in_specs=[smem, vmem, vmem, hbm], out_specs=(vmem, vmem, vmem),
            scratch_shapes=[VMEM((pieces * plen, 2 * hd), BF16), VMEM((n, 2 * plen, 2 * plen), BF16),
                            VMEM((2 * plen, hd), BF16), VMEM((2 * plen, hd), BF16), VMEM((2 * plen, 128), F32),
                            VMEM((2 * plen, 128), F32), VMEM((2 * plen, hd), F32), pltpu.SemaphoreType.DMA((pieces,))],
            compiler_params=pltpu.CompilerParams(vmem_limit_bytes=44 * 1024 * 1024),
            name='query_side',
        )(meta, a_loc, docs, g_all)
        ld_all, y_out = exchange(ld, o_loc, wo, n, hd, 3)
        dk_loc, dv_loc = pl.pallas_call(
            functools.partial(key_kernel, pieces, plen, hd, scale),
            out_shape=(jax.ShapeDtypeStruct((tok, hd), BF16), jax.ShapeDtypeStruct((tok, hd), BF16)),
            in_specs=[smem, vmem, vmem, vmem, hbm], out_specs=(vmem, vmem),
            scratch_shapes=[VMEM((3, 2, 2 * plen, hd), BF16), VMEM((plen, hd), BF16), VMEM((plen, hd), BF16),
                            VMEM((plen, hd), F32), VMEM((plen, hd), F32), pltpu.SemaphoreType.DMA((3, 4))],
            compiler_params=pltpu.CompilerParams(vmem_limit_bytes=16 * 1024 * 1024),
            name='key_side',
        )(meta, a_loc, docs, ld_all, g_all)
        nt = (((1,), (1,)), ((), ()))
        dx = (lax.dot_general(dq_loc, wq, nt, preferred_element_type=F32)
              + lax.dot_general(dk_loc, wk, nt, preferred_element_type=F32)
              + lax.dot_general(dv_loc, wv, nt, preferred_element_type=F32))
        return y_out, dx.astype(BF16)

    return jax.shard_map(local_layer, mesh=mesh,
                         in_specs=(row_spec, row_spec, row_spec, full_spec, full_spec, full_spec, full_spec),
                         out_specs=(row_spec, row_spec), check_vma=False)
```

```python
import collections
import functools
import heapq
import math
import random

import jax
import jax.numpy as jnp
from jax import lax
from jax.experimental import pallas as pl
from jax.experimental.pallas import tpu as pltpu
from jax.sharding import PartitionSpec as P

NEG_BIG = -1.0e30
MESH = pl.DeviceIdType.MESH
VMEM = pltpu.VMEM
F32 = jnp.float32
REACHES = (20, 16, 11)
TUNES = ((1.05, 0.3, 52), (1.05, 1.0, 15), (1.2, 3.0, 49), (1.2, 3.0, 29))
PARTS = 2
BF16 = jnp.bfloat16


def remote(src, dst, send_sem, recv_sem, dev):
    return pltpu.make_async_remote_copy(src_ref=src, dst_ref=dst, send_sem=send_sem, recv_sem=recv_sem,
                                        device_id={'cp': dev}, device_id_type=MESH)


def exchange_kernel(n, hd, ld_ref, o_ref, wo_ref, all_ref, y_ref, wo_v, y_v, load_sem, store_sem, send_sem, recv_sem, own_sem):
    me = lax.axis_index('cp')
    barrier = pltpu.get_barrier_semaphore()
    load = pltpu.make_async_copy(wo_ref, wo_v, load_sem)
    load.start()

    def greet(off, _):
        pl.semaphore_signal(barrier, inc=1, device_id={'cp': lax.rem(me + off, n)}, device_id_type=MESH)
        return 0
    lax.fori_loop(1, n, greet, 0)
    own = pltpu.make_async_copy(ld_ref, all_ref.at[me], own_sem)
    own.start()
    pl.semaphore_wait(barrier, n - 1)

    def send(off, _):
        remote(ld_ref, all_ref.at[me], send_sem.at[off], recv_sem.at[off], lax.rem(me + off, n)).start()
        return 0
    lax.fori_loop(1, n, send, 0)
    load.wait()
    cols = 2 * hd
    count = y_ref.shape[1] // cols

    def store(j):
        at = pl.ds(pl.multiple_of(j * cols, cols), cols)
        return pltpu.make_async_copy(y_v.at[:, at], y_ref.at[:, at], store_sem.at[j])

    def column(j, _):
        at = pl.ds(pl.multiple_of(j * cols, cols), cols)
        y_v[:, at] = dot_nn(o_ref[...], wo_v[:, at]).astype(BF16)
        store(j).start()
        return 0
    lax.fori_loop(0, count, column, 0)
    own.wait()

    def settle(off, _):
        src = lax.rem(me + n - off, n)
        copy = remote(ld_ref, all_ref.at[src], send_sem.at[off], recv_sem.at[off], lax.rem(me + off, n))
        copy.wait_send()
        copy.wait_recv()
        return 0
    lax.fori_loop(1, n, settle, 0)

    def stored(j, _):
        store(j).wait()
        return 0
    lax.fori_loop(0, count, stored, 0)


def exchange(ld, o, wo, n, hd, cid):
    tok, d_model = o.shape[0], wo.shape[1]
    vmem, hbm = pl.BlockSpec(memory_space=VMEM), pl.BlockSpec(memory_space=pltpu.HBM)
    dma = pltpu.SemaphoreType.DMA
    return pl.pallas_call(
        functools.partial(exchange_kernel, n, hd),
        out_shape=(jax.ShapeDtypeStruct((n,) + ld.shape, ld.dtype), jax.ShapeDtypeStruct((tok, d_model), BF16)),
        in_specs=[vmem, vmem, hbm], out_specs=(vmem, hbm),
        scratch_shapes=[VMEM(wo.shape, BF16), VMEM((tok, d_model), BF16), dma, dma((d_model // (2 * hd),)), dma((n,)), dma((n,)), dma],
        compiler_params=pltpu.CompilerParams(collective_id=cid, has_side_effects=True, vmem_limit_bytes=16 * 1024 * 1024),
        name='exchange',
    )(ld, o, wo)


def project_kernel(n, hd, doc_ref, x_ref, dy_ref, wk_ref, wv_ref, wq_ref, wo_ref, out_ref, docs_ref,
                   x_v, dy_v, kv_v, wq_v, wo_v, load_sem, send_sem, recv_sem, own_sem):
    me = lax.axis_index('cp')
    barrier = pltpu.get_barrier_semaphore()

    def greet(off, _):
        pl.semaphore_signal(barrier, inc=1, device_id={'cp': lax.rem(me + off, n)}, device_id_type=MESH)
        return 0
    lax.fori_loop(1, n, greet, 0)
    loads = [pltpu.make_async_copy(src, dst, load_sem.at[i]) for i, (src, dst) in enumerate(
        ((x_ref, x_v), (wk_ref, kv_v.at[0]), (wv_ref, kv_v.at[1]), (wq_ref, wq_v), (dy_ref, dy_v), (wo_ref, wo_v)))]
    for load in loads:
        load.start()
    own = pltpu.make_async_copy(doc_ref, docs_ref.at[me], own_sem)
    own.start()
    half = x_ref.shape[0] // 2

    def fill(kind, src, weights, dot, col):
        def rows(t, _):
            out_ref[jnp.abs(t - kind), :, pl.ds(col, hd)] = dot(src[pl.ds(t * half, half), :], weights).astype(BF16)
            return 0
        lax.fori_loop(0, 2, rows, 0)

    loads[0].wait()
    for i in range(2):
        loads[1 + i].wait()
        fill(0, x_v, kv_v[i], dot_nn, i * hd)
    pl.semaphore_wait(barrier, n - 1)

    def send(off, _):
        remote(doc_ref, docs_ref.at[me], send_sem.at[off], recv_sem.at[off], lax.rem(me + off, n)).start()
        return 0
    lax.fori_loop(1, n, send, 0)
    loads[3].wait()
    for h in range(2):
        fill(1, x_v, wq_v[:, pl.ds(h * hd, hd)], dot_nn, (2 + h) * hd)
    loads[4].wait()
    loads[5].wait()
    for h in range(2):
        fill(1, dy_v, wo_v[pl.ds(h * hd, hd), :], dot_nt, (4 + h) * hd)
    own.wait()

    def settle(off, _):
        src = lax.rem(me + n - off, n)
        copy = remote(doc_ref, docs_ref.at[src], send_sem.at[off], recv_sem.at[off], lax.rem(me + off, n))
        copy.wait_send()
        copy.wait_recv()
        return 0
    lax.fori_loop(1, n, settle, 0)


def project(doc, x, dy, wk, wv, wq, wo, n, cid):
    tok, d_model = x.shape
    hd = wk.shape[1]
    vmem, hbm = pl.BlockSpec(memory_space=VMEM), pl.BlockSpec(memory_space=pltpu.HBM)
    return pl.pallas_call(
        functools.partial(project_kernel, n, hd),
        out_shape=(jax.ShapeDtypeStruct((2, tok // 2, 6 * hd), BF16), jax.ShapeDtypeStruct((n,) + doc.shape, doc.dtype)),
        in_specs=[vmem] + [hbm] * 6, out_specs=(vmem, vmem),
        scratch_shapes=[VMEM((tok, d_model), BF16), VMEM((tok, d_model), BF16), VMEM((2, d_model, hd), BF16),
                        VMEM((d_model, 2 * hd), BF16), VMEM((2 * hd, d_model), BF16), pltpu.SemaphoreType.DMA((6,)),
                        pltpu.SemaphoreType.DMA((n,)), pltpu.SemaphoreType.DMA((n,)), pltpu.SemaphoreType.DMA],
        compiler_params=pltpu.CompilerParams(collective_id=cid, has_side_effects=True, vmem_limit_bytes=48 * 1024 * 1024),
        name='project',
    )(doc, x, dy, wk, wv, wq, wo)


def small_gather(x, n, cid):
    return pl.pallas_call(
        functools.partial(small_gather_kernel, n),
        out_shape=jax.ShapeDtypeStruct((n,) + x.shape, x.dtype),
        in_specs=[pl.BlockSpec(memory_space=VMEM)],
        out_specs=pl.BlockSpec(memory_space=VMEM),
        scratch_shapes=[pltpu.SemaphoreType.DMA((n,)), pltpu.SemaphoreType.DMA((n,)), pltpu.SemaphoreType.DMA],
        compiler_params=pltpu.CompilerParams(collective_id=cid, has_side_effects=True),
        name=f'small_gather_{cid}',
    )(x)


def needs(side, reach):
    chips = side * side
    last = 4 * chips - 1
    out = {}
    for dev in range(2 * chips):
        for s in (0, 1):
            kv, qd = (dev, last - dev) if s == 0 else (last - dev, dev)
            out[dev, s] = {k for k in range(chips) for c in (2 * k, 2 * k + 1, last - 2 * k, last - 2 * k - 1)
                           if k != dev // 2 and (0 < c - kv <= reach or 0 < qd - c <= reach)}
    return out


def neighbours(side, chip):
    x, y = chip % side, chip // side
    return ((y * side + (x + 1) % side, 0), (y * side + (x - 1) % side, 1),
            ((y + 1) % side * side + x, 2), ((y - 1) % side * side + x, 3))


def grow(side, load, src, targets, steep, hop):
    depth = {src: 0}
    edges = []
    missing = set(targets)
    while missing:
        dist = {c: depth[c] * hop for c in depth}
        back = {}
        heap = sorted((d, c) for c, d in dist.items())
        done = set()
        while True:
            d, c = heapq.heappop(heap)
            if c in done:
                continue
            done.add(c)
            if c in missing:
                break
            for nb, way in neighbours(side, c):
                w = d + steep ** load[c, way] + hop
                if nb not in depth and w < dist.get(nb, 1e30):
                    dist[nb], back[nb] = w, (c, way)
                    heapq.heappush(heap, (w, nb))
        path = []
        while c not in depth:
            path.append((back[c][0], back[c][1], c))
            c = back[c][0]
        for p, way, c in reversed(path):
            depth[c] = depth[p] + 1
            edges.append((p, way, c))
            missing.discard(c)
    return edges, depth


def unit_key(side, depth, src, chip, s, h):
    return depth, (src // side - chip // side) % side, (src % side - chip % side) % side, s, h


def arrivals(side, trees, order, hold, lag):
    todo = collections.defaultdict(list)
    for (dev, s, h), (edges, depth) in trees.items():
        onward = collections.defaultdict(list)
        for p, way, c in edges:
            onward[p].append((way, c))
        for c in depth:
            key = unit_key(side, depth[c], dev // 2, c, s, h)
            todo[c, dev % 2].append((order(key), key, (dev, s, h), onward[c]))
    came = {(dev // 2, (dev, s, h)): 0.0 for dev, s, h in trees}
    clock, free, seen = collections.Counter(), collections.Counter(), collections.defaultdict(list)
    queues = {place: sorted(v, key=lambda u: u[:2], reverse=True) for place, v in todo.items()}
    moved = True
    while moved:
        moved = False
        for place, queue in queues.items():
            while queue and (place[0], queue[-1][2]) in came:
                _, key, unit, onward = queue.pop()
                clock[place] = max(clock[place], came[place[0], unit])
                seen[key].append(came[place[0], unit])
                for way, c in onward:
                    free[place, way] = max(clock[place], free[place, way]) + hold
                    came[c, unit] = free[place, way] + lag
                moved = True
    return max(came.values()), {k: sum(v) / len(v) for k, v in seen.items()}


def plan(side, reach, parts, tune):
    steep, hop, seed = tune
    nd = needs(side, reach)
    keys = [(dev, s, h) for h in range(parts) for dev in range(2 * side * side) for s in (0, 1)]
    random.Random(seed).shuffle(keys)
    load, trees, best = collections.Counter(), {}, None
    for _ in range(6):
        for key in keys:
            for p, way, c in trees.get(key, ((), ()))[0]:
                load[p, way] -= 1
            trees[key] = grow(side, load, key[0] // 2, nd[key[0], key[1]], steep, hop)
            for p, way, c in trees[key][0]:
                load[p, way] += 1
        mean = {}
        for _ in range(5):
            end, later = arrivals(side, trees, lambda k: (k[0], round(mean.get(k, 0.0), 3)), 16.9 / parts, 2.5)
            if best is None or end < best[0]:
                best = end, dict(trees), mean
            mean = later
    units = collections.defaultdict(lambda: dict(take=0, send=[0] * 4, keep=0, given=0))
    for (dev, s, h), (edges, depth) in best[1].items():
        src, core = dev // 2, dev % 2

        def unit(c):
            return units[unit_key(side, depth[c], src, c, s, h)]
        for p, way, c in edges:
            unit(c)['take'] |= 1 << (2 * c + core)
            unit(p)['send'][way] |= 1 << (2 * p + core)
        for c in nd[dev, s] | {src}:
            unit(c)['keep'] |= 1 << (2 * c + core)
            unit(c)['given'] |= 1 << (2 * c + 1 - core)
    order = sorted(units.items(), key=lambda kv: (kv[0][0], round(best[2].get(kv[0], 0.0), 3), kv[0]))
    return [(k, v['take'], v['send'], v['keep'], v['given']) for k, v in order]


def multicast_kernel(side, parts, units, x_ref, out_ref, send_sem, recv_sem, chip_send, chip_recv, own_sem):
    me = lax.axis_index('cp')
    core = lax.rem(me, 2)
    chip = me // 2
    cx, cy = lax.rem(chip, side), chip // side
    rows = x_ref.shape[1] // parts
    bit = lax.shift_left(jnp.int32(1), me.astype(jnp.int32))

    def among(mask):
        mask = mask - (1 << 32) if mask >> 31 else mask
        return (bit & jnp.int32(mask)) != 0

    def dev(y, x, c):
        return (lax.rem(cy + y + side, side) * side + lax.rem(cx + x + side, side)) * 2 + c

    partner = dev(0, 0, 1 - core)
    ways = (dev(0, 1, core), dev(0, -1, core), dev(1, 0, core), dev(-1, 0, core))
    barrier = pltpu.get_barrier_semaphore()
    for peer in ways + (partner,):
        pl.semaphore_signal(barrier, inc=1, device_id={'cp': peer}, device_id_type=MESH)
    own = pltpu.make_async_copy(x_ref, out_ref.at[me], own_sem)
    own.start()
    pl.semaphore_wait(barrier, 5)

    sends = []
    slot = {key: k for k, (key, *_) in enumerate(units)}
    for k, ((depth, dy, dx, s, h), take, send, keep, given) in enumerate(units):
        mine = dy == 0 and dx == 0
        block = pl.ds(h * rows, rows)
        here = out_ref.at[dev(dy, dx, core), s, block]
        src = x_ref.at[s, block] if mine else here

        def push():
            for way, mask in enumerate(send):
                if mask:
                    ahead = (dy - (0, 0, 1, -1)[way]) % side, (dx - (1, -1, 0, 0)[way]) % side
                    copy = remote(src, here, send_sem.at[len(sends)], recv_sem.at[slot[depth + 1, *ahead, s, h]], ways[way])
                    sends.append((mask, copy))
                    pl.when(among(mask))(copy.start)
            if keep:
                copy = remote(src, here, chip_send.at[k], chip_recv.at[k], partner)
                sends.append((keep, copy))
                pl.when(among(keep))(copy.start)
        if take:
            pl.when(among(take))(remote(here, here, send_sem.at[0], recv_sem.at[k], partner).wait_recv)
        push()
    for k, ((_, dy, dx, s, h), take, send, keep, given) in enumerate(units):
        there = out_ref.at[dev(dy, dx, 1 - core), s, pl.ds(h * rows, rows)]
        if given:
            pl.when(among(given))(remote(there, there, chip_send.at[k], chip_recv.at[k], partner).wait_recv)
    for mask, copy in sends:
        pl.when(among(mask))(copy.wait_send)
    own.wait()


def multicast(x, n, reach, tune, parts, cid):
    side = math.isqrt(n // 2)
    units = plan(side, reach, parts, tune)
    count = sum(1 for u in units for m in u[2] if m) + len(units)
    sems = [pltpu.SemaphoreType.DMA((c,)) for c in (count, len(units), len(units), len(units))]
    return pl.pallas_call(
        functools.partial(multicast_kernel, side, parts, units),
        out_shape=jax.ShapeDtypeStruct((n,) + x.shape, x.dtype),
        in_specs=[pl.BlockSpec(memory_space=VMEM)],
        out_specs=pl.BlockSpec(memory_space=pltpu.HBM),
        scratch_shapes=sems + [pltpu.SemaphoreType.DMA],
        compiler_params=pltpu.CompilerParams(collective_id=cid, has_side_effects=True, vmem_limit_bytes=8 * 1024 * 1024),
        name=f'multicast_{reach}',
    )(x)


def dot_nt(a, b):
    return lax.dot_general(a, b, (((1,), (1,)), ((), ())), preferred_element_type=F32)


def dot_nn(a, b):
    return lax.dot_general(a, b, (((1,), (0,)), ((), ())), preferred_element_type=F32)


def column(row):
    return jnp.transpose(jnp.broadcast_to(row.astype(F32), (128, row.shape[1])))[:, 0:1].astype(jnp.int32)


def query_kernel(pieces, plen, hd, scale, meta, a_ref, docs_ref, g_ref, o_ref, dq_ref, ld_ref,
                 kv, p_s, q2, do2, m_s, l_s, acc, sem):
    wide = 2 * plen
    for t in range(2):
        c, lo = meta[t], meta[2 + t]
        blocks = (c - lo + 2) // 2

        def fetch(i):
            p = jnp.minimum(lo + i, c)
            far = (p >= pieces // 2).astype(jnp.int32)
            d = jnp.where(far == 1, pieces - 1 - p, p)
            return pltpu.make_async_copy(g_ref.at[d, far, :, pl.ds(0, 2 * hd)], kv.at[pl.ds(i * plen, plen)], sem.at[i])

        def issue(i, _):
            fetch(i).start()
            return 0
        lax.fori_loop(0, 2 * blocks, issue, 0)
        for h in range(2):
            rows = pl.ds(h * plen, plen)
            q2[rows, :] = a_ref[1 - t, :, pl.ds((2 + h) * hd, hd)]
            do2[rows, :] = a_ref[1 - t, :, pl.ds((4 + h) * hd, hd)]
        m_s[...] = jnp.full_like(m_s, NEG_BIG)
        l_s[...] = jnp.zeros_like(l_s)
        acc[...] = jnp.zeros_like(acc)
        doc = column(docs_ref[pl.ds(c, 1), :])
        doc = jnp.concatenate([doc, doc], axis=0)
        row = lax.broadcasted_iota(jnp.int32, (plen, 1), 0) + c * plen
        row = jnp.concatenate([row, row], axis=0)

        def keys(i):
            return pl.ds(pl.multiple_of(i * wide, wide), wide)

        def scores(i):
            s = dot_nt(q2[...], kv[keys(i), pl.ds(0, hd)]) * scale
            p = lo + 2 * i
            key_doc = jnp.concatenate([docs_ref[pl.ds(p, 1), :], docs_ref[pl.ds(jnp.minimum(p + 1, c), 1), :]], axis=1)
            col = lax.broadcasted_iota(jnp.int32, (1, wide), 1) + p * plen
            return jnp.where((key_doc == doc) & (col <= row), s, NEG_BIG)

        def sweep_norm(i, _):
            fetch(2 * i).wait()
            fetch(2 * i + 1).wait()
            s = scores(i)
            parts = [s[:, k:k + 128] for k in range(0, wide, 128)]
            m = m_s[...]
            m_new = jnp.maximum(m, functools.reduce(jnp.maximum, parts))
            l_s[...] = l_s[...] * jnp.exp(m - m_new) + sum(jnp.exp(part - m_new) for part in parts)
            m_s[...] = m_new
            return 0
        lax.fori_loop(0, blocks, sweep_norm, 0)
        top = jnp.max(m_s[...], axis=1, keepdims=True)
        total = jnp.sum(l_s[...] * jnp.exp(m_s[...] - top), axis=1, keepdims=True)
        log_norm = top + jnp.log(total)

        def sweep_out(i, _):
            p = jnp.exp(scores(i) - log_norm).astype(BF16)
            p_s[i] = p
            acc[...] += dot_nn(p, kv[keys(i), pl.ds(hd, hd)])
            return 0
        lax.fori_loop(0, blocks, sweep_out, 0)
        out = acc[...].astype(BF16)
        delta = jnp.sum(do2[...].astype(F32) * out.astype(F32), axis=1, keepdims=True)
        acc[...] = jnp.zeros_like(acc)

        def sweep_dq(i, _):
            dp = dot_nt(do2[...], kv[keys(i), pl.ds(hd, hd)])
            ds = (p_s[i].astype(F32) * (dp - delta)).astype(BF16)
            acc[...] += dot_nn(ds, kv[keys(i), pl.ds(0, hd)])
            return 0
        lax.fori_loop(0, blocks, sweep_dq, 0)
        dq = (acc[...] * scale).astype(BF16)
        for h in range(2):
            o_ref[pl.ds(t * plen, plen), pl.ds(h * hd, hd)] = out[h * plen:(h + 1) * plen]
            dq_ref[pl.ds(t * plen, plen), pl.ds(h * hd, hd)] = dq[h * plen:(h + 1) * plen]
        ld_ref[pl.ds(2 * t, 1), :] = jnp.transpose(jnp.broadcast_to(log_norm, (wide, 128)))[0:1]
        ld_ref[pl.ds(2 * t + 1, 1), :] = jnp.transpose(jnp.broadcast_to(delta, (wide, 128)))[0:1]


def key_kernel(pieces, plen, hd, scale, meta, a_ref, docs_ref, ld_ref, g_ref, dk_ref, dv_ref,
               qd, kt, vt, dk_acc, dv_acc, sem):
    for t in range(2):
        c, hi = meta[t], meta[4 + t]
        count = hi - c + 1

        def place(i):
            p = c + i
            far = (p >= pieces // 2).astype(jnp.int32)
            return p, far, jnp.where(far == 1, pieces - 1 - p, p)

        def fetch(i):
            _, far, d = place(i)
            b = lax.rem(i, 3)
            return [pltpu.make_async_copy(g_ref.at[d, 1 - far, :, pl.ds((2 + k) * hd, hd)],
                                          qd.at[b, k // 2, pl.ds((k % 2) * plen, plen)], sem.at[b, k]) for k in range(4)]

        def start(i):
            for copy in fetch(i):
                copy.start()

        start(0)
        pl.when(count > 1)(lambda: start(1))
        kt[...] = a_ref[t, :, pl.ds(0, hd)]
        vt[...] = a_ref[t, :, pl.ds(hd, hd)]
        dk_acc[...] = jnp.zeros_like(dk_acc)
        dv_acc[...] = jnp.zeros_like(dv_acc)
        doc = column(docs_ref[pl.ds(c, 1), :])
        key = lax.broadcasted_iota(jnp.int32, (plen, 1), 0)

        def sweep(i, _):
            pl.when(i + 2 < count)(lambda: start(i + 2))
            for copy in fetch(i):
                copy.wait()
            b = lax.rem(i, 3)
            p_idx, far, d = place(i)
            col = lax.broadcasted_iota(jnp.int32, (1, plen), 1) + i * plen
            seen = (docs_ref[pl.ds(p_idx, 1), :] == doc) & (col >= key)
            seen = jnp.concatenate([seen, seen], axis=1)
            st = jnp.where(seen, dot_nt(kt[...], qd[b, 0]) * scale, NEG_BIG)
            dpt = dot_nt(vt[...], qd[b, 1])
            pt = jnp.exp(st - ld_ref[d, pl.ds(2 * far, 1), :]).astype(BF16)
            dst = (pt.astype(F32) * (dpt - ld_ref[d, pl.ds(2 * far + 1, 1), :])).astype(BF16)
            dv_acc[...] += dot_nn(pt, qd[b, 1])
            dk_acc[...] += dot_nn(dst, qd[b, 0])
            return 0
        lax.fori_loop(0, count, sweep, 0)
        dk_ref[pl.ds(t * plen, plen), :] = (dk_acc[...] * scale).astype(BF16)
        dv_ref[pl.ds(t * plen, plen), :] = dv_acc[...].astype(BF16)


def solution(mesh):
    n = mesh.shape['cp']
    row_spec = P(('dp', 'cp'))
    full_spec = P()

    def local_layer(x_in, dy_in, doc_id, w_q, w_k, w_v, w_o):
        tok, d_model = x_in.shape
        heads, hd = w_q.shape[1], w_q.shape[2]
        plen = tok // 2
        pieces = 2 * n
        seq = tok * n
        scale = hd ** -0.5
        me = lax.axis_index('cp')
        wq = w_q.reshape(d_model, heads * hd)
        wk = w_k.reshape(d_model, hd)
        wv = w_v.reshape(d_model, hd)
        wo = w_o.reshape(heads * hd, d_model)

        lane = 128
        doc_rows = doc_id.reshape(tok // lane, lane)
        a_loc, docs = project(doc_rows, x_in, dy_in, wk, wv, wq, wo, n, 1)
        docs = docs.reshape(n, 2, plen)
        docs = jnp.concatenate([docs[:, 0], docs[::-1, 1]])
        first, last = docs[:, 0], docs[:, plen - 1]
        begun = jnp.sum((last[None, :] < first[:, None]).astype(jnp.int32), axis=1)
        opens, closes = (f(doc_rows.reshape(2, plen // lane, lane), axis=(1, 2)) for f in (jnp.min, jnp.max))
        meta = jnp.concatenate([
            jnp.stack([me, pieces - 1 - me]).astype(jnp.int32),
            jnp.sum((last[None, :] < opens[:, None]).astype(jnp.int32), axis=1),
            jnp.sum((first[None, :] <= closes[:, None]).astype(jnp.int32), axis=1) - 1])
        span = jnp.max(jnp.arange(pieces) - begun)
        level = sum((span <= r).astype(jnp.int32) for r in REACHES)
        g_all = lax.switch(level, [functools.partial(multicast, n=n, reach=r, tune=TUNES[i], parts=PARTS, cid=4 + i)
                                   for i, r in enumerate((pieces,) + REACHES)], a_loc)

        smem = pl.BlockSpec(memory_space=pltpu.SMEM)
        vmem = pl.BlockSpec(memory_space=VMEM)
        hbm = pl.BlockSpec(memory_space=pltpu.HBM)
        o_loc, dq_loc, ld = pl.pallas_call(
            functools.partial(query_kernel, pieces, plen, hd, scale),
            out_shape=(jax.ShapeDtypeStruct((tok, heads * hd), BF16), jax.ShapeDtypeStruct((tok, heads * hd), BF16),
                       jax.ShapeDtypeStruct((4, 2 * plen), F32)),
            in_specs=[smem, vmem, vmem, hbm], out_specs=(vmem, vmem, vmem),
            scratch_shapes=[VMEM((pieces * plen, 2 * hd), BF16), VMEM((n, 2 * plen, 2 * plen), BF16),
                            VMEM((2 * plen, hd), BF16), VMEM((2 * plen, hd), BF16), VMEM((2 * plen, 128), F32),
                            VMEM((2 * plen, 128), F32), VMEM((2 * plen, hd), F32), pltpu.SemaphoreType.DMA((pieces,))],
            compiler_params=pltpu.CompilerParams(vmem_limit_bytes=44 * 1024 * 1024),
            name='query_side',
        )(meta, a_loc, docs, g_all)
        ld_all, y_out = exchange(ld, o_loc, wo, n, hd, 3)
        dk_loc, dv_loc = pl.pallas_call(
            functools.partial(key_kernel, pieces, plen, hd, scale),
            out_shape=(jax.ShapeDtypeStruct((tok, hd), BF16), jax.ShapeDtypeStruct((tok, hd), BF16)),
            in_specs=[smem, vmem, vmem, vmem, hbm], out_specs=(vmem, vmem),
            scratch_shapes=[VMEM((3, 2, 2 * plen, hd), BF16), VMEM((plen, hd), BF16), VMEM((plen, hd), BF16),
                            VMEM((plen, hd), F32), VMEM((plen, hd), F32), pltpu.SemaphoreType.DMA((3, 4))],
            compiler_params=pltpu.CompilerParams(vmem_limit_bytes=16 * 1024 * 1024),
            name='key_side',
        )(meta, a_loc, docs, ld_all, g_all)
        nt = (((1,), (1,)), ((), ()))
        dx = (lax.dot_general(dq_loc, wq, nt, preferred_element_type=F32)
              + lax.dot_general(dk_loc, wk, nt, preferred_element_type=F32)
              + lax.dot_general(dv_loc, wv, nt, preferred_element_type=F32))
        return y_out, dx.astype(BF16)

    return jax.shard_map(local_layer, mesh=mesh,
                         in_specs=(row_spec, row_spec, row_spec, full_spec, full_spec, full_spec, full_spec),
                         out_specs=(row_spec, row_spec), check_vma=False)
```
